16 devices in a mesh: ens: 2 (over y, z), feat: 8 (over x, core).
Axes of the slice: x: 4, y: 2, z: 1, core: 2. Of those that a mesh axis runs over, the one named last changes fastest.
The devices are a block of a 4x4x8 slice.
Arguments:
- particles: float32 [1024, 32768], P('ens', 'feat'), parts along dimension 0
- prec_diag: float32 [65536], P(('ens', 'feat')), parts along dimension 0
- low_factor: bfloat16 [65536, 32], P(('ens', 'feat')), parts along dimension 0
- prior_mean: float32 [65536], P(('ens', 'feat')), parts along dimension 0
- data_mat: bfloat16 [2048, 32768], P('ens', 'feat'), parts along dimension 0
- labels: int32 [2048], P('ens'), parts along dimension 0
Outputs:
- output: float32 [1024, 32768], P('ens', 'feat'), parts along dimension 0
There are 2 independent parts. The reference program is written for one: setup_inputs(seed, part) draws one part's arguments, and reference() takes and returns one part's arrays. A program takes and returns all parts, laid end to end along the dimension named above; each array names one.
All inputs are finite; a program needn't handle non-finite values.
Results may differ from the reference program's by a relative error of at most 0.001.
Values are sent between devices in bfloat16 or wider.
A program may use at most 768 MiB of HBM per device.

```python
import math
import jax
import jax.numpy as jnp

FEAT_DIM = 32768
LOW_RANK = 32
PARTICLES = 512
DATA_ROWS = 1024
NUM_STEPS = 3


def setup_inputs(seed: int = 0, part: int = 0) -> dict:
    base_key = jax.random.fold_in(jax.random.key(seed), part)
    sub_keys = jax.random.split(base_key, 8)
    common = jax.random.normal(sub_keys[0], (1, FEAT_DIM), jnp.float32)
    spread = jax.random.uniform(sub_keys[1], (PARTICLES, 1), jnp.float32, 0.5, 1.5)
    noise_mat = jax.random.normal(sub_keys[2], (PARTICLES, FEAT_DIM), jnp.float32)
    particles = common + spread * noise_mat
    prec_diag = jnp.exp(jax.random.uniform(sub_keys[3], (FEAT_DIM,), jnp.float32, -1.0, 1.0)) / FEAT_DIM
    u_scale = 1.1 * (FEAT_DIM * math.sqrt(LOW_RANK * FEAT_DIM)) ** -0.5
    low_factor = (jax.random.normal(sub_keys[4], (FEAT_DIM, LOW_RANK), jnp.float32) * u_scale).astype(jnp.bfloat16)
    prior_mean = 0.5 * jax.random.normal(sub_keys[5], (FEAT_DIM,), jnp.float32)
    data_scale = 1.5 / math.sqrt(FEAT_DIM)
    data_mat = (jax.random.normal(sub_keys[6], (DATA_ROWS, FEAT_DIM), jnp.float32) * data_scale).astype(jnp.bfloat16)
    labels = jax.random.randint(sub_keys[7], (DATA_ROWS,), 0, 2, jnp.int32)
    return {"particles": particles, "prec_diag": prec_diag, "low_factor": low_factor,
            "prior_mean": prior_mean, "data_mat": data_mat, "labels": labels}


def reference(particles, prec_diag, low_factor, prior_mean, data_mat, labels):
    band_width = 2.0 * FEAT_DIM
    step_size = FEAT_DIM / 4.0
    lik_weight = 2.0 / math.sqrt(DATA_ROWS * FEAT_DIM)
    targets = labels.astype(jnp.float32)[None, :]
    state = particles
    for step_idx in range(NUM_STEPS):
        part_bf = state.astype(jnp.bfloat16)
        centred = state - prior_mean
        projected = jnp.dot(centred.astype(jnp.bfloat16), low_factor, preferred_element_type=jnp.float32)
        gram_mat = jnp.dot(part_bf, part_bf.T, preferred_element_type=jnp.float32)
        sq_norm = jnp.diagonal(gram_mat)
        sq_dist = jnp.maximum(sq_norm[:, None] + sq_norm[None, :] - 2.0 * gram_mat, 0.0)
        kernel = jnp.exp(-sq_dist / band_width)
        logits = jnp.dot(part_bf, data_mat.T, preferred_element_type=jnp.float32)
        residual = targets - jax.nn.sigmoid(logits)
        low_rank = jnp.dot(projected.astype(jnp.bfloat16), low_factor.T, preferred_element_type=jnp.float32)
        lik_term = jnp.dot(residual.astype(jnp.bfloat16), data_mat, preferred_element_type=jnp.float32)
        log_grad = lik_weight * lik_term - centred * prec_diag - low_rank
        kern_bf = kernel.astype(jnp.bfloat16)
        driving = jnp.dot(kern_bf, log_grad.astype(jnp.bfloat16), preferred_element_type=jnp.float32)
        pulled = jnp.dot(kern_bf, part_bf, preferred_element_type=jnp.float32)
        row_sum = jnp.sum(kernel, axis=1, keepdims=True)
        update_dir = (driving + (2.0 / band_width) * (row_sum * state - pulled)) / PARTICLES
        state = state + step_size * update_dir
    return state
```

```python
import functools
import math
import jax
import jax.numpy as jnp
from jax import lax
from jax.experimental import pallas as pl
from jax.experimental.pallas import tpu as pltpu
from jax.sharding import PartitionSpec as P

NUM_STEPS = 3
CORES = 2
F32, BF16 = jnp.float32, jnp.bfloat16
NN = (((1,), (0,)), ((), ()))
NT = (((1,), (1,)), ((), ()))
MESH = pl.DeviceIdType.MESH
KINDS = ("d2d", "s1a", "s1b", "ownb", "owna", "reda", "redb",
         "gr", "gl", "gp", "fa", "flp", "fb", "frp", "fop")


def dot(a, b, dims=NN):
    return lax.dot_general(a, b, dims, preferred_element_type=F32)


class Sum:
    def __init__(self, rows, half, width, part, pair, send, recv, full, sems, where, finish):
        self.rows, self.half, self.width = rows, half, width
        self.part, self.pair, self.send, self.recv, self.full = part, pair, send, recv, full
        self.ssem, self.rsem = sems
        self.core, self.chip, self.chips = where
        self.finish = finish

    def chip_at(self, hop):
        return lax.rem(self.chip + hop + self.chips, self.chips)

    def row(self, chip, core=None):
        core = self.core if core is None else core
        return pl.multiple_of((core * self.chips + chip) * self.rows, 8)

    def copy(self, kind, ch):
        rows, half = self.rows, self.half
        core, chip, chips = self.core, self.chip, self.chips
        right, left, opp = self.chip_at(1), self.chip_at(-1), self.chip_at(2)
        me = lambda c: {"feat": c * CORES + core}
        pair = {"feat": chip * CORES + (1 - core)}
        snd, rcv, full = self.send.at[ch], self.recv.at[ch], self.full.at[ch]
        block = lambda ref, lo, hi: ref.at[pl.ds(lo, hi - lo), :]

        def same(lo, size):
            ref = full.at[pl.ds(lo, size), :]
            return ref, ref
        if kind == "d2d":
            size = self.chips * rows
            src = self.part.at[ch].at[pl.ds(pl.multiple_of((1 - core) * size, 8), size), :]
            dst, dev = self.pair.at[ch], pair
        elif kind == "s1a":
            src, dst, dev = block(snd, 0, half), block(rcv, 0, half), me(right)
        elif kind == "s1b":
            src, dst, dev = block(snd, half, rows), block(rcv, half, rows), me(left)
        elif kind == "ownb":
            src, dst, dev = block(snd, rows + half, 2 * rows), block(rcv, rows + half, 2 * rows), me(right)
        elif kind == "owna":
            src, dst, dev = block(snd, 2 * rows, 2 * rows + half), block(rcv, 2 * rows, 2 * rows + half), me(left)
        elif kind == "reda":
            src, dst, dev = block(snd, rows, rows + half), block(rcv, rows, rows + half), me(right)
        elif kind == "redb":
            src, dst, dev = block(snd, 2 * rows + half, 3 * rows), block(rcv, 2 * rows + half, 3 * rows), me(left)
        elif kind == "gr":
            (src, dst), dev = same(self.row(chip), rows), me(right)
        elif kind == "gl":
            (src, dst), dev = same(self.row(chip), rows), me(left)
        elif kind == "gp":
            (src, dst), dev = same(self.row(chip), rows), pair
        elif kind == "fa":
            (src, dst), dev = same(self.row(left), half), me(right)
        elif kind == "flp":
            (src, dst), dev = same(self.row(left), rows), pair
        elif kind == "fb":
            (src, dst), dev = same(self.row(right) + half, rows - half), me(left)
        elif kind == "frp":
            (src, dst), dev = same(self.row(right), rows), pair
        elif kind == "fop":
            (src, dst), dev = same(self.row(opp), rows), pair
        k = KINDS.index(kind)
        return pltpu.make_async_remote_copy(
            src_ref=src, dst_ref=dst, send_sem=self.ssem.at[ch, k], recv_sem=self.rsem.at[ch, k],
            device_id=dev, device_id_type=MESH)

    def start(self, kind, ch):
        self.copy(kind, ch).start()

    def wait(self, kind, ch):
        self.copy(kind, ch).wait_recv()

    def mine(self, ch, chip, lo, hi):
        a = self.part[ch, pl.ds(self.row(chip) + lo, hi - lo), :]
        b = self.pair[ch, pl.ds(pl.multiple_of(chip * self.rows, 8) + lo, hi - lo), :]
        return a + b

    def put(self, ch, lo, value):
        self.send[ch, lo:lo + value.shape[0], :] = value.astype(self.send.dtype)

    def got(self, ch, lo, hi):
        return self.recv[ch, lo:hi, :].astype(F32)

    def stage(self, n, ch):
        rows, half = self.rows, self.half
        right, left, opp = self.chip_at(1), self.chip_at(-1), self.chip_at(2)
        if n == 0:
            self.start("d2d", ch)
        elif n == 1:
            self.wait("d2d", ch)
            self.put(ch, 0, self.mine(ch, opp, 0, rows))
            self.start("s1a", ch)
            self.start("s1b", ch)
            self.put(ch, rows + half, self.mine(ch, right, half, rows))
            self.start("ownb", ch)
            self.put(ch, 2 * rows, self.mine(ch, left, 0, half))
            self.start("owna", ch)
        elif n == 2:
            self.wait("s1a", ch)
            self.put(ch, rows, self.mine(ch, right, 0, half) + self.got(ch, 0, half))
            self.start("reda", ch)
            self.wait("s1b", ch)
            self.put(ch, 2 * rows + half, self.mine(ch, left, half, rows) + self.got(ch, half, rows))
            self.start("redb", ch)
        elif n == 3:
            for kind in ("ownb", "owna", "reda", "redb"):
                self.wait(kind, ch)
            total = self.mine(ch, self.chip, 0, rows) + self.got(ch, rows, 2 * rows) + self.got(ch, 2 * rows, 3 * rows)
            self.full[ch, pl.ds(self.row(self.chip), rows), :] = self.finish(ch, total)
            for kind in ("gr", "gl", "gp"):
                self.start(kind, ch)
        elif n == 4:
            self.wait("gr", ch)
            self.start("fa", ch)
            self.start("flp", ch)
            self.wait("gl", ch)
            self.start("fb", ch)
            self.start("frp", ch)
        elif n == 5:
            self.wait("fa", ch)
            self.wait("fb", ch)
            self.start("fop", ch)
        elif n == 6:
            for kind in ("gp", "flp", "frp", "fop"):
                self.wait(kind, ch)

    def drain(self, ch):
        for kind in KINDS:
            self.copy(kind, ch).wait_send()


def kernel(cfg, theta_hbm, lam_ref, mu_ref, ut_ref, a_hbm, y_ref, out_hbm,
           th, tb, av, sa, sb, kb, kv,
           zpart, zpair, zsend, zrecv, zfull, gpart, gpair, gsend, grecv, gfull,
           load_sem, store_sem, zss, zrs, gss, grs):
    chips, band, step, lik = cfg
    n_part, dim = th.shape
    m_rows = av.shape[0]
    nb = n_part // 2
    mc = m_rows // 2
    own = nb // (CORES * chips)
    tile = 1024
    rank = ut_ref.shape[0]
    me = lax.axis_index("feat")
    core, chip = lax.rem(me, CORES), me // CORES
    where = (core, chip, chips)

    def finish_z(ch, z):
        y = y_ref[:, (ch % 2) * mc:(ch % 2 + 1) * mc]
        return (y - 1.0 / (1.0 + jnp.exp(-z))).astype(BF16)

    zs = Sum(own, own // 2, mc, zpart, zpair, zsend, zrecv, zfull, (zss, zrs), where, finish_z)
    gs = Sum(own + 8, own // 2, nb, gpart, gpair, gsend, grecv, gfull, (gss, grs), where, lambda ch, g: g)

    def load_theta(i):
        return pltpu.make_async_copy(theta_hbm.at[pl.ds(i * nb, nb), :], th.at[pl.ds(i * nb, nb), :], load_sem.at[i])

    def load_a(j):
        return pltpu.make_async_copy(a_hbm.at[pl.ds(j * mc, mc), :], av.at[pl.ds(j * mc, mc), :], load_sem.at[2 + j])

    load_theta(0).start()
    load_a(0).start()
    load_theta(1).start()
    load_a(1).start()

    barrier = pltpu.get_barrier_semaphore()
    peers = (chip * CORES + (1 - core), zs.chip_at(1) * CORES + core, zs.chip_at(-1) * CORES + core)
    for peer in peers:
        pl.semaphore_signal(barrier, inc=1, device_id={"feat": peer}, device_id_type=MESH)

    gpart[...] = jnp.zeros_like(gpart)
    pl.semaphore_wait(barrier, len(peers))

    def tiles(body, width=tile):
        @pl.loop(0, dim // width)
        def _(t):
            body(pl.ds(pl.multiple_of(t * width, width), width))

    def rows(i):
        return slice(i * nb, (i + 1) * nb)

    def prep(i):
        load_theta(i).wait()

        def body(n):
            tb[rows(i), n] = th[rows(i), n].astype(BF16)
        tiles(body)

    def project(i):
        def body(t, acc):
            n = pl.ds(pl.multiple_of(t * tile, tile), tile)
            x = (th[rows(i), n] - mu_ref[:, n]).astype(BF16)
            return acc + dot(x, ut_ref[:, n], NT)
        q = lax.fori_loop(0, dim // tile, body, jnp.zeros((nb, rank), F32))
        ch = 2 * i
        fold = own // 8
        for o in range(CORES * chips):
            parts = [q[o * own + 8 * k:o * own + 8 * (k + 1)] for k in range(fold)]
            gpart[ch, o * (own + 8) + own:(o + 1) * (own + 8), 0:fold * rank] = jnp.concatenate(parts, axis=1)

    def gram(i):
        for j in range(i + 1):
            g = dot(tb[rows(i), :], tb[rows(j), :], NT)
            for o in range(CORES * chips):
                gpart[i + j, o * (own + 8):o * (own + 8) + own, :] = g[o * own:(o + 1) * own]

    def logit(i, j):
        zpart[2 * i + j] = dot(tb[rows(i), :], av[j * mc:(j + 1) * mc, :], NT)

    def low_rank(i):
        ch = 2 * i
        fold = own // 8
        parts = []
        for o in range(CORES * chips):
            p = gfull[ch, o * (own + 8) + own:(o + 1) * (own + 8), 0:128]
            parts += [p[:, rank * k:rank * (k + 1)] for k in range(fold)]
        q = jnp.concatenate(parts, axis=0).astype(BF16)

        def body(n):
            x = th[rows(i), n] - mu_ref[:, n]
            sa[rows(i), n] = -(x * lam_ref[:, n]) - dot(q, ut_ref[:, n])
        tiles(body)

    def lik_first(i):
        def body(n):
            sa[rows(i), n] = sa[rows(i), n] + lik * dot(zfull[2 * i], av[0:mc, n])
        tiles(body)

    def lik_last(i):
        def body(n):
            sb[rows(i), n] = (sa[rows(i), n] + lik * dot(zfull[2 * i + 1], av[mc:2 * mc, n])).astype(BF16)
        tiles(body)

    def kernel_mat():
        def gblock(ch):
            return jnp.concatenate(
                [gfull[ch, o * (own + 8):o * (own + 8) + own, :] for o in range(CORES * chips)], axis=0)

        def diag(g):
            eye = lax.broadcasted_iota(jnp.int32, g.shape, 0) == lax.broadcasted_iota(jnp.int32, g.shape, 1)
            d = jnp.where(eye, g, 0.0)
            return jnp.sum(d, axis=1, keepdims=True), jnp.sum(d, axis=0, keepdims=True)

        def rbf(c, r, g):
            return jnp.exp(-jnp.maximum(c + r - 2.0 * g, 0.0) / band)
        g00, g10, g11 = gblock(0), gblock(1), gblock(2)
        c0, r0 = diag(g00)
        c1, r1 = diag(g11)
        k00, k10, k11 = rbf(c0, r0, g00), rbf(c1, r0, g10), rbf(c1, r1, g11)
        k01 = k10.T
        kb[0:nb, 0:nb] = k00.astype(BF16)
        kb[0:nb, nb:] = k01.astype(BF16)
        kb[nb:, 0:nb] = k10.astype(BF16)
        kb[nb:, nb:] = k11.astype(BF16)
        kv[0:nb] = jnp.sum(k00, axis=1, keepdims=True) + jnp.sum(k01, axis=1, keepdims=True)
        kv[nb:] = jnp.sum(k10, axis=1, keepdims=True) + jnp.sum(k11, axis=1, keepdims=True)

    def pull(i):
        def body(n):
            t = th[rows(i), n]
            th[rows(i), n] = t + (step / n_part) * ((2.0 / band) * (kv[rows(i)] * t - dot(kb[rows(i), :], tb[:, n])))
        tiles(body)

    def drive(i, out=None):
        def body(n):
            t = th[rows(i), n] + (step / n_part) * dot(kb[rows(i), :], sb[:, n])
            th[rows(i), n] = t
            if out is None:
                tb[rows(i), n] = t.astype(BF16)
            else:
                out(n).start()
        tiles(body)

    def store(i):
        def out(n):
            return pltpu.make_async_copy(th.at[rows(i), n], out_hbm.at[rows(i), n], store_sem.at[i])
        return out

    @pl.loop(0, NUM_STEPS)
    def _(s):
        @pl.when(s == 0)
        def _():
            prep(0)
        project(0)
        gram(0)
        gs.stage(0, 0)

        @pl.when(s == 0)
        def _():
            load_a(0).wait()
        logit(0, 0)
        zs.stage(0, 0)
        gs.stage(1, 0)

        @pl.when(s == 0)
        def _():
            load_a(1).wait()
        logit(0, 1)
        zs.stage(0, 1)
        zs.stage(1, 0)
        gs.stage(2, 0)

        @pl.when(s == 0)
        def _():
            prep(1)

        @pl.when(s > 0)
        def _():
            drive(1)
        zs.stage(1, 1)
        zs.stage(2, 0)
        project(1)
        gs.stage(3, 0)
        gram(1)
        gs.stage(0, 1)
        gs.stage(0, 2)
        zs.stage(2, 1)
        zs.stage(3, 0)
        logit(1, 0)
        zs.stage(0, 2)
        gs.stage(1, 1)
        gs.stage(1, 2)
        gs.stage(4, 0)
        zs.stage(3, 1)
        logit(1, 1)
        zs.stage(0, 3)
        zs.stage(1, 2)
        gs.stage(2, 1)
        gs.stage(2, 2)
        zs.stage(4, 0)
        gs.stage(5, 0)
        gs.stage(6, 0)
        low_rank(0)
        zs.stage(1, 3)
        zs.stage(4, 1)
        gs.stage(3, 1)
        gs.stage(3, 2)
        zs.stage(5, 0)
        zs.stage(6, 0)
        lik_first(0)
        zs.stage(2, 2)
        zs.stage(2, 3)
        gs.stage(4, 1)
        gs.stage(4, 2)
        zs.stage(5, 1)
        zs.stage(6, 1)
        lik_last(0)
        zs.stage(3, 2)
        zs.stage(3, 3)
        gs.stage(5, 1)
        gs.stage(5, 2)
        gs.stage(6, 1)
        gs.stage(6, 2)
        low_rank(1)
        zs.stage(4, 2)
        kernel_mat()
        zs.stage(4, 3)
        zs.stage(5, 2)
        pull(0)
        zs.stage(5, 3)
        zs.stage(6, 2)
        pull(1)
        lik_first(1)
        zs.stage(6, 3)
        lik_last(1)
        for ch in range(4):
            zs.drain(ch)
        for ch in range(3):
            gs.drain(ch)

        @pl.when(s < NUM_STEPS - 1)
        def _():
            drive(0)

    drive(0, store(0))
    drive(1, store(1))
    for i in range(2):
        for t in range(dim // tile):
            store(i)(pl.ds(t * tile, tile)).wait()


def solution(mesh):
    feat_size = mesh.shape["feat"]
    chips = feat_size // CORES

    def local_run(particles, prec_diag, low_factor, prior_mean, data_mat, labels):
        n_part, dim = particles.shape
        m_rows = data_mat.shape[0]
        rank = low_factor.shape[1]
        dim_full = dim * feat_size
        cfg = (chips, 2.0 * dim_full, dim_full / 4.0, 2.0 / math.sqrt(m_rows * dim_full))
        nb, mc = n_part // 2, m_rows // 2
        own = nb // feat_size
        vm, any_ = pl.BlockSpec(memory_space=pltpu.VMEM), pl.BlockSpec(memory_space=pl.ANY)
        dma = pltpu.SemaphoreType.DMA
        scratch = [
            pltpu.VMEM((n_part, dim), F32), pltpu.VMEM((n_part, dim), BF16), pltpu.VMEM((m_rows, dim), BF16),
            pltpu.VMEM((n_part, dim), F32), pltpu.VMEM((n_part, dim), BF16),
            pltpu.VMEM((n_part, n_part), BF16), pltpu.VMEM((n_part, 1), F32),
        ]
        for count, rows, width, wire in ((4, own, mc, BF16), (3, own + 8, nb, F32)):
            scratch += [
                pltpu.VMEM((count, feat_size * rows, width), F32), pltpu.VMEM((count, chips * rows, width), F32),
                pltpu.VMEM((count, 3 * rows, width), wire), pltpu.VMEM((count, 3 * rows, width), wire),
                pltpu.VMEM((count, feat_size * rows, width), wire),
            ]
        scratch += [dma((4,)), dma((2,))] + [dma((4, len(KINDS)))] * 2 + [dma((3, len(KINDS)))] * 2
        return pl.pallas_call(
            functools.partial(kernel, cfg),
            out_shape=jax.ShapeDtypeStruct((n_part, dim), F32),
            in_specs=[any_, vm, vm, vm, any_, vm],
            out_specs=any_,
            scratch_shapes=scratch,
            compiler_params=pltpu.CompilerParams(
                collective_id=0, has_side_effects=True, vmem_limit_bytes=60 * 2**20),
            cost_estimate=pl.CostEstimate(flops=60 * 10**9, bytes_accessed=32 * 2**20, transcendentals=0),
        )(particles, prec_diag[None, :], prior_mean[None, :], low_factor.T, data_mat, labels.astype(F32)[None, :])

    return jax.shard_map(
        local_run,
        mesh=mesh,
        in_specs=(P("ens", "feat"), P(("ens", "feat")), P(("ens", "feat"), None),
                  P(("ens", "feat")), P("ens", "feat"), P("ens")),
        out_specs=P("ens", "feat"),
        check_vma=False,
    )
```

```python
import functools
import math
import jax
import jax.numpy as jnp
from jax import lax
from jax.experimental import pallas as pl
from jax.experimental.pallas import tpu as pltpu
from jax.sharding import PartitionSpec as P

NUM_STEPS = 3
CORES = 2
LANES = 128
F32, BF16 = jnp.float32, jnp.bfloat16
NN = (((1,), (0,)), ((), ()))
NT = (((1,), (1,)), ((), ()))
MESH = pl.DeviceIdType.MESH
KINDS = ("d2d", "s1a", "s1b", "ownb", "owna", "reda", "redb",
         "gr", "gl", "gp", "fa", "flp", "fb", "frp", "fop")
DIRECT_KINDS = ("d2d", "ir", "il", "io", "gr", "gl", "go", "gp", "flp", "frp", "fop")
CHUNKS = ("g0", "z0", "z3", "g1", "z1", "z2")
DIRECT = ('g0', 'g1', 'z0', 'z1', 'z2', 'z3')
SCHEDULE = (
    "z0q", "z3:0", "z0p", "z0:0", "z3:1", "gram0", "g0:0", "drive1a", "z0:1", "drive1b", "g0:1", "z1",
    "z1:0", "proj1", "z3:3", "gram1", "z0:3", "proj0", "z1:1", "g1:0", "z2", "g1:1", "z0:4", "z2:0",
    "z3:4", "z3:5", "z1:3", "z0:5", "z3:6", "z0:6", "z2:1", "g1:3", "z1:4", "z1:5", "z2:3", "z1:6",
    "l0a", "g0:3", "l0b", "g1:4", "g1:5", "lf1a", "lf1b", "z2:4", "z2:5", "g1:6", "lr0", "lr1",
    "g0:4", "z2:6", "g0:5", "ll1a", "ll1b", "g0:6", "kmat", "drive0a", "drive0b",
)


def dot(a, b, dims=NN):
    return lax.dot_general(a, b, dims, preferred_element_type=F32)


class Chunk:
    def __init__(self, name, bufs, where, finish):
        self.part, self.pair, self.send, self.recv, self.full, self.ssem, self.rsem = bufs
        self.core, self.chip, self.chips = where
        self.rows = self.full.shape[0] // (CORES * self.chips)
        self.half = self.rows // 32 * 16
        self.direct = name in DIRECT
        self.kinds = DIRECT_KINDS if self.direct else KINDS
        self.finish = finish

    def chip_at(self, hop):
        return lax.rem(self.chip + hop + self.chips, self.chips)

    def row(self, chip):
        return pl.multiple_of((self.core * self.chips + chip) * self.rows, 8)

    def copy(self, kind):
        rows, half = self.rows, self.half
        core, chip = self.core, self.chip
        right, left, opp = self.chip_at(1), self.chip_at(-1), self.chip_at(2)
        at = lambda c: {"feat": c * CORES + core}
        pair = {"feat": chip * CORES + (1 - core)}
        snd, rcv, full = self.send, self.recv, self.full

        def same(lo, size):
            ref = full.at[pl.ds(lo, size), :]
            return ref, ref

        def slot(lo, hi):
            return snd.at[pl.ds(lo, hi - lo), :], rcv.at[pl.ds(lo, hi - lo), :]

        if kind == "d2d":
            size = self.chips * rows
            src, dst = self.part.at[pl.ds(pl.multiple_of((1 - core) * size, 8), size), :], self.pair
            dev = pair
        else:
            (src, dst), dev = {
                "s1a": lambda: (slot(0, half), at(right)),
                "s1b": lambda: (slot(half, rows), at(left)),
                "ownb": lambda: (slot(rows + half, 2 * rows), at(right)),
                "owna": lambda: (slot(2 * rows, 2 * rows + half), at(left)),
                "reda": lambda: (slot(rows, rows + half), at(right)),
                "redb": lambda: (slot(2 * rows + half, 3 * rows), at(left)),
                "io": lambda: (slot(0, rows), at(opp)),
                "ir": lambda: (slot(rows, 2 * rows), at(right)),
                "il": lambda: (slot(2 * rows, 3 * rows), at(left)),
                "gr": lambda: (same(self.row(chip), rows), at(right)),
                "gl": lambda: (same(self.row(chip), rows), at(left)),
                "go": lambda: (same(self.row(chip), rows), at(opp)),
                "gp": lambda: (same(self.row(chip), rows), pair),
                "fa": lambda: (same(self.row(left), half), at(right)),
                "flp": lambda: (same(self.row(left), rows), pair),
                "fb": lambda: (same(self.row(right) + half, rows - half), at(left)),
                "frp": lambda: (same(self.row(right), rows), pair),
                "fop": lambda: (same(self.row(opp), rows), pair),
            }[kind]()
        k = self.kinds.index(kind)
        return pltpu.make_async_remote_copy(
            src_ref=src, dst_ref=dst, send_sem=self.ssem.at[k], recv_sem=self.rsem.at[k],
            device_id=dev, device_id_type=MESH)

    def start(self, *kinds):
        for kind in kinds:
            self.copy(kind).start()

    def wait(self, *kinds):
        for kind in kinds:
            self.copy(kind).wait_recv()

    def mine(self, chip, lo, hi):
        a = self.part[pl.ds(self.row(chip) + lo, hi - lo), :]
        b = self.pair[pl.ds(pl.multiple_of(chip * self.rows, 8) + lo, hi - lo), :]
        return a + b

    def put(self, lo, value):
        self.send[lo:lo + value.shape[0], :] = value.astype(self.send.dtype)

    def got(self, lo, hi):
        return self.recv[lo:hi, :].astype(F32)

    def stage(self, n):
        rows, half = self.rows, self.half
        right, left, opp = self.chip_at(1), self.chip_at(-1), self.chip_at(2)
        if n == 0:
            self.start("d2d")
        elif n == 1:
            self.wait("d2d")
            self.put(0, self.mine(opp, 0, rows))
            if self.direct:
                self.start("io")
                self.put(rows, self.mine(right, 0, rows))
                self.start("ir")
                self.put(2 * rows, self.mine(left, 0, rows))
                self.start("il")
            else:
                self.start("s1a", "s1b")
                self.put(rows + half, self.mine(right, half, rows))
                self.start("ownb")
                self.put(2 * rows, self.mine(left, 0, half))
                self.start("owna")
        elif n == 2:
            self.wait("s1a")
            self.put(rows, self.mine(right, 0, half) + self.got(0, half))
            self.start("reda")
            self.wait("s1b")
            self.put(2 * rows + half, self.mine(left, half, rows) + self.got(half, rows))
            self.start("redb")
        elif n == 3:
            total = self.mine(self.chip, 0, rows)
            if self.direct:
                self.wait("ir", "il", "io")
                total = total + self.got(rows, 2 * rows) + self.got(2 * rows, 3 * rows) + self.got(0, rows)
            else:
                self.wait("ownb", "owna", "reda", "redb")
                total = total + self.got(rows, 2 * rows) + self.got(2 * rows, 3 * rows)
            self.full[pl.ds(self.row(self.chip), rows), :] = self.finish(total)
            if self.direct:
                self.start("go")
            self.start("gr", "gl", "gp")
        elif n == 4:
            self.wait("gr")
            if not self.direct:
                self.start("fa")
            self.start("flp")
            self.wait("gl")
            if not self.direct:
                self.start("fb")
            self.start("frp")
        elif n == 5:
            if self.direct:
                self.wait("go")
            else:
                self.wait("fa", "fb")
            self.start("fop")
        elif n == 6:
            self.wait("gp", "flp", "frp", "fop")

    def drain(self):
        for kind in self.kinds:
            self.copy(kind).wait_send()


def kernel(cfg, theta_hbm, lam_ref, mu_ref, ut_ref, a_hbm, y_ref, out_hbm, th, tb, av, sa, sb, kb, kv,
           load_sem, store_sem, *chunk_bufs):
    chips, band, step, lik = cfg
    n_part, dim = th.shape
    m_rows = av.shape[0]
    nb, mc = n_part // 2, m_rows // 2
    owners = CORES * chips
    own = nb // owners
    wide, sub = dim // 2, 512
    rank = ut_ref.shape[0]
    pack = LANES // rank
    pull = 2.0 / band
    gain = step / n_part
    me = lax.axis_index("feat")
    where = (lax.rem(me, CORES), me // CORES, chips)

    def finish(name):
        if name[0] == "g":
            return lambda g: g
        lo = 0 if name in ("z0", "z1") else mc

        def residual(z):
            return (y_ref[:, lo:lo + mc].astype(F32) - 1.0 / (1.0 + jnp.exp(-z))).astype(BF16)
        return residual

    ch = {}
    for k, name in enumerate(CHUNKS):
        ch[name] = Chunk(name, chunk_bufs[7 * k:7 * k + 7], where, finish(name))

    def rows(i):
        return slice(i * nb, (i + 1) * nb)

    def load_theta(i):
        return pltpu.make_async_copy(theta_hbm.at[pl.ds(i * nb, nb), :], th.at[pl.ds(i * nb, nb), :], load_sem.at[i])

    def load_a(j):
        return pltpu.make_async_copy(a_hbm.at[pl.ds(j * mc, mc), :], av.at[pl.ds(j * mc, mc), :], load_sem.at[2 + j])

    load_theta(0).start()
    load_a(0).start()
    load_a(1).start()
    load_theta(1).start()

    any_chunk = ch[CHUNKS[0]]
    barrier = pltpu.get_barrier_semaphore()
    peers = [where[1] * CORES + (1 - where[0])]
    peers += [any_chunk.chip_at(hop) * CORES + where[0] for hop in (1, -1, 2)]
    for peer in peers:
        pl.semaphore_signal(barrier, inc=1, device_id={"feat": peer}, device_id_type=MESH)
    pl.semaphore_wait(barrier, len(peers))

    def columns(lo, hi):
        return [slice(n, n + sub) for n in range(lo, hi, sub)]

    def prep(i):
        load_theta(i).wait()

        @pl.loop(0, dim // wide)
        def _(t):
            n = pl.ds(pl.multiple_of(t * wide, wide), wide)
            tb[rows(i), n] = th[rows(i), n].astype(BF16)

    def project(i):
        q = jnp.zeros((nb, rank), F32)
        for n in columns(0, dim):
            q = q + dot((th[rows(i), n] - mu_ref[:, n]).astype(BF16), ut_ref[:, n], NT)
        piece = 2 * own + 8
        for o in range(owners):
            parts = [q[o * own + 8 * k:o * own + 8 * (k + 1)] for k in range(pack)]
            ch["g1"].part[o * piece + 2 * own:(o + 1) * piece, i * LANES:(i + 1) * LANES] = \
                jnp.concatenate(parts, axis=1)

    def gram(i):
        g = dot(tb[rows(i), :], tb[0:(i + 1) * nb, :], NT)
        part = ch[f"g{i}"].part
        piece = part.shape[0] // owners
        for j in range(i + 1):
            for o in range(owners):
                part[o * piece + j * own:o * piece + (j + 1) * own, :] = g[o * own:(o + 1) * own, j * nb:(j + 1) * nb]

    def logit(name, i, j):
        ch[name].part[...] = dot(tb[rows(i), :], av[j * mc:(j + 1) * mc, :], NT)

    def base(i, n, q):
        t = th[rows(i), n]
        return -((t - mu_ref[:, n]) * lam_ref[:, n]) - dot(q, ut_ref[:, n]) - pull * tb[rows(i), n].astype(F32)

    def gathered_q(i):
        piece = 2 * own + 8
        parts = []
        for o in range(owners):
            p = ch["g1"].full[o * piece + 2 * own:(o + 1) * piece, i * LANES:(i + 1) * LANES]
            parts += [p[:, rank * k:rank * (k + 1)] for k in range(pack)]
        return jnp.concatenate(parts, axis=0).astype(BF16)

    def both_lik(lo, hi):
        for n in columns(lo, hi):
            sa[rows(0), n] = lik * (dot(ch["z0"].full[...], av[0:mc, n]) + dot(ch["z3"].full[...], av[mc:2 * mc, n]))

    def first_lik(lo, hi):
        for n in columns(lo, hi):
            sa[rows(1), n] = lik * dot(ch["z1"].full[...], av[0:mc, n])

    def last_lik(lo, hi):
        for n in columns(lo, hi):
            sb[rows(1), n] = (sa[rows(1), n] + lik * dot(ch["z2"].full[...], av[mc:2 * mc, n])).astype(BF16)

    def low_rank(i):
        q = gathered_q(i)
        for n in columns(0, dim):
            s = sa[rows(i), n] + base(i, n, q)
            if i == 0:
                sb[rows(i), n] = s.astype(BF16)
            else:
                sa[rows(i), n] = s

    def kernel_mat():
        def block(name, j):
            full = ch[name].full
            piece = full.shape[0] // owners
            return jnp.concatenate(
                [full[o * piece + j * own:o * piece + (j + 1) * own, :] for o in range(owners)], axis=0)

        def diag(g):
            eye = lax.broadcasted_iota(jnp.int32, g.shape, 0) == lax.broadcasted_iota(jnp.int32, g.shape, 1)
            d = jnp.where(eye, g, 0.0)
            return jnp.sum(d, axis=1, keepdims=True), jnp.sum(d, axis=0, keepdims=True)

        def rbf(c, r, g):
            return jnp.exp(-jnp.maximum(c + r - 2.0 * g, 0.0) / band)

        g00, g10, g11 = block("g0", 0), block("g1", 0), block("g1", 1)
        (c0, r0), (c1, r1) = diag(g00), diag(g11)
        k00, k10, k11 = rbf(c0, r0, g00), rbf(c1, r0, g10), rbf(c1, r1, g11)
        k01 = k10.T
        for i, j, k in ((0, 0, k00), (0, 1, k01), (1, 0, k10), (1, 1, k11)):
            kb[rows(i), rows(j)] = k.astype(BF16)
        for i, pair in ((0, (k00, k01)), (1, (k10, k11))):
            total = jnp.sum(pair[0], axis=1, keepdims=True) + jnp.sum(pair[1], axis=1, keepdims=True)
            kv[rows(i), :] = jnp.broadcast_to(gain * pull * total, (nb, LANES))

    def drive(i, lo, hi, out=False):
        for n in columns(lo, hi):
            t = th[rows(i), n]
            scale = jnp.concatenate([kv[rows(i), :]] * (sub // LANES), axis=1)
            t = t + (scale * t + gain * dot(kb[rows(i), :], sb[:, n]))
            th[rows(i), n] = t
            if not out:
                tb[rows(i), n] = t.astype(BF16)

    def store(i, lo, hi):
        n = pl.ds(lo, hi - lo)
        return pltpu.make_async_copy(th.at[rows(i), n], out_hbm.at[rows(i), n], store_sem.at[2 * i + lo // (hi - lo)])

    halves = {"a": (0, wide), "b": (wide, dim)}
    pieces = {
        "proj0": lambda: project(0), "proj1": lambda: project(1), "gram0": lambda: gram(0), "gram1": lambda: gram(1),
        "z0p": lambda: logit("z0", 0, 0), "z0q": lambda: logit("z3", 0, 1),
        "z1": lambda: logit("z1", 1, 0), "z2": lambda: logit("z2", 1, 1),
        "lr0": lambda: low_rank(0), "lr1": lambda: low_rank(1), "kmat": kernel_mat,
    }
    for h, (lo, hi) in halves.items():
        pieces["l0" + h] = functools.partial(both_lik, lo, hi)
        pieces["lf1" + h] = functools.partial(first_lik, lo, hi)
        pieces["ll1" + h] = functools.partial(last_lik, lo, hi)
        pieces["drive0" + h] = functools.partial(drive, 0, lo, hi)
        pieces["drive1" + h] = functools.partial(drive, 1, lo, hi)

    @pl.loop(0, NUM_STEPS)
    def _(s):
        @pl.when(s == 0)
        def _():
            prep(0)

        loaded = set()
        for item in SCHEDULE:
            if ":" in item:
                name, n = item.split(":")
                ch[name].stage(int(n))
                continue
            if item in ("z0p", "z0q"):
                @pl.when(s == 0)
                def _():
                    load_a("pq".index(item[-1])).wait()
            if item == "drive1a":
                @pl.when(s == 0)
                def _():
                    prep(1)
            if item[:6] == "drive1":
                pl.when(s > 0)(pieces[item])
            elif item[:6] == "drive0":
                pl.when(s < NUM_STEPS - 1)(pieces[item])
            else:
                pieces[item]()
        for name in CHUNKS:
            ch[name].drain()

    for i in range(2):
        for lo, hi in halves.values():
            drive(i, lo, hi, out=True)
            store(i, lo, hi).start()
    for i in range(2):
        for lo, hi in halves.values():
            store(i, lo, hi).wait()


def solution(mesh):
    feat_size = mesh.shape["feat"]
    chips = feat_size // CORES

    def local_run(particles, prec_diag, low_factor, prior_mean, data_mat, labels):
        n_part, dim = particles.shape
        m_rows = data_mat.shape[0]
        dim_full = dim * feat_size
        cfg = (chips, 2.0 * dim_full, dim_full / 4.0, 2.0 / math.sqrt(m_rows * dim_full))
        nb, mc = n_part // 2, m_rows // 2
        own = nb // feat_size
        vm, any_ = pl.BlockSpec(memory_space=pltpu.VMEM), pl.BlockSpec(memory_space=pl.ANY)
        dma = pltpu.SemaphoreType.DMA
        scratch = [
            pltpu.VMEM((n_part, dim), F32), pltpu.VMEM((n_part, dim), BF16), pltpu.VMEM((m_rows, dim), BF16),
            pltpu.VMEM((n_part, dim), F32), pltpu.VMEM((n_part, dim), BF16),
            pltpu.VMEM((n_part, n_part), BF16), pltpu.VMEM((n_part, LANES), F32), dma((4,)), dma((4,)),
        ]
        for name in CHUNKS:
            wire, width, rows = (F32, nb, own) if name[0] == "g" else (BF16, mc, own)
            if name == "g1":
                rows = 2 * own + 8
            count = len(DIRECT_KINDS if name in DIRECT else KINDS)
            scratch += [
                pltpu.VMEM((feat_size * rows, width), F32), pltpu.VMEM((chips * rows, width), F32),
                pltpu.VMEM((3 * rows, width), wire), pltpu.VMEM((3 * rows, width), wire),
                pltpu.VMEM((feat_size * rows, width), wire), dma((count,)), dma((count,)),
            ]
        return pl.pallas_call(
            functools.partial(kernel, cfg),
            out_shape=jax.ShapeDtypeStruct((n_part, dim), F32),
            in_specs=[any_, vm, vm, vm, any_, vm],
            out_specs=any_,
            scratch_shapes=scratch,
            compiler_params=pltpu.CompilerParams(
                collective_id=0, has_side_effects=True, vmem_limit_bytes=60 * 2**20),
            cost_estimate=pl.CostEstimate(flops=60 * 10**9, bytes_accessed=32 * 2**20, transcendentals=0),
        )(particles, prec_diag[None, :], prior_mean[None, :], low_factor.T, data_mat, labels[None, :])

    return jax.shard_map(
        local_run,
        mesh=mesh,
        in_specs=(P("ens", "feat"), P(("ens", "feat")), P(("ens", "feat"), None),
                  P(("ens", "feat")), P("ens", "feat"), P("ens")),
        out_specs=P("ens", "feat"),
        check_vma=False,
    )
```

```python
import functools
import math
import jax
import jax.numpy as jnp
from jax import lax
from jax.experimental import pallas as pl
from jax.experimental.pallas import tpu as pltpu
from jax.sharding import PartitionSpec as P

NUM_STEPS = 3
CORES = 2
LANES = 128
F32, BF16 = jnp.float32, jnp.bfloat16
NN = (((1,), (0,)), ((), ()))
NT = (((1,), (1,)), ((), ()))
LOGICAL = pl.DeviceIdType.LOGICAL
KINDS = ("d2d", "s1a", "s1b", "ownb", "owna", "reda", "redb",
         "gr", "gl", "gp", "fa", "flp", "fb", "frp", "fop")
DIRECT_KINDS = ("d2d", "ir", "il", "io", "gr", "gl", "go", "gp", "flp", "frp", "fop")
CHUNKS = ("g0", "z0", "z3", "g1", "z1", "z2")
DIRECT = ('g0', 'g1', 'z0', 'z1', 'z2', 'z3')
SCHEDULE = (
    "z0q", "z3:0", "z0p", "z0:0", "z3:1", "gram0", "z0:1", "g0:0", "drive1a", "drive1b", "g0:1", "z1",
    "z3:3", "z1:0", "gram1", "z0:3", "proj", "g1:0", "z1:1", "g1:1", "z3:4", "z3:5", "z2", "z0:4",
    "z1:3", "z0:5", "z2:0", "z2:1", "z3:6", "g1:3", "z0:6", "z1:4", "l0a", "z2:3", "g0:3", "z1:5",
    "l0b", "z1:6", "lf1a", "lf1b", "g1:4", "g1:5", "z2:4", "z2:5", "g1:6", "lr1", "z2:6", "ll1a",
    "g0:4", "g0:5", "ll1b", "lr0", "g0:6", "kmat", "drive0a", "drive0b",
)


def dot(a, b, dims=NN):
    return lax.dot_general(a, b, dims, preferred_element_type=F32)


class Chunk:
    def __init__(self, name, bufs, where, finish):
        self.part, self.pair, self.send, self.recv, self.full, self.ssem, self.rsem = bufs
        self.core, self.chip, self.chips, self.chip_of, self.ids = where
        self.rows = self.full.shape[0] // (CORES * self.chips)
        self.half = self.rows // 32 * 16
        self.direct = name in DIRECT
        self.kinds = DIRECT_KINDS if self.direct else KINDS
        self.finish = finish

    def row(self, hop):
        return pl.multiple_of((self.core * self.chips + self.chip_of[hop]) * self.rows, 8)

    def copy(self, kind):
        rows, half = self.rows, self.half
        core, pair = self.core, self.ids["pair"]
        chip, right, left, opp = 0, 1, -1, 2
        at = lambda hop: self.ids[hop]
        snd, rcv, full = self.send, self.recv, self.full

        def same(lo, size):
            ref = full.at[pl.ds(lo, size), :]
            return ref, ref

        def slot(lo, hi):
            return snd.at[pl.ds(lo, hi - lo), :], rcv.at[pl.ds(lo, hi - lo), :]

        if kind == "d2d":
            size = self.chips * rows
            src, dst = self.part.at[pl.ds(pl.multiple_of((1 - core) * size, 8), size), :], self.pair
            dev = pair
        else:
            (src, dst), dev = {
                "s1a": lambda: (slot(0, half), at(right)),
                "s1b": lambda: (slot(half, rows), at(left)),
                "ownb": lambda: (slot(rows + half, 2 * rows), at(right)),
                "owna": lambda: (slot(2 * rows, 2 * rows + half), at(left)),
                "reda": lambda: (slot(rows, rows + half), at(right)),
                "redb": lambda: (slot(2 * rows + half, 3 * rows), at(left)),
                "io": lambda: (slot(0, rows), at(opp)),
                "ir": lambda: (slot(rows, 2 * rows), at(right)),
                "il": lambda: (slot(2 * rows, 3 * rows), at(left)),
                "gr": lambda: (same(self.row(chip), rows), at(right)),
                "gl": lambda: (same(self.row(chip), rows), at(left)),
                "go": lambda: (same(self.row(chip), rows), at(opp)),
                "gp": lambda: (same(self.row(chip), rows), pair),
                "fa": lambda: (same(self.row(left), half), at(right)),
                "flp": lambda: (same(self.row(left), rows), pair),
                "fb": lambda: (same(self.row(right) + half, rows - half), at(left)),
                "frp": lambda: (same(self.row(right), rows), pair),
                "fop": lambda: (same(self.row(opp), rows), pair),
            }[kind]()
        k = self.kinds.index(kind)
        return pltpu.make_async_remote_copy(
            src_ref=src, dst_ref=dst, send_sem=self.ssem.at[k], recv_sem=self.rsem.at[k],
            device_id=dev, device_id_type=LOGICAL)

    def start(self, *kinds):
        for kind in kinds:
            self.copy(kind).start()

    def wait(self, *kinds):
        for kind in kinds:
            self.copy(kind).wait_recv()

    def mine(self, hop, lo, hi):
        a = self.part[pl.ds(self.row(hop) + lo, hi - lo), :]
        b = self.pair[pl.ds(pl.multiple_of(self.chip_of[hop] * self.rows, 8) + lo, hi - lo), :]
        return a + b

    def put(self, lo, value):
        self.send[lo:lo + value.shape[0], :] = value.astype(self.send.dtype)

    def got(self, lo, hi):
        return self.recv[lo:hi, :].astype(F32)

    def stage(self, n):
        rows, half = self.rows, self.half
        right, left, opp = 1, -1, 2
        if n == 0:
            self.start("d2d")
        elif n == 1:
            self.wait("d2d")
            self.put(0, self.mine(opp, 0, rows))
            if self.direct:
                self.start("io")
                self.put(rows, self.mine(right, 0, rows))
                self.start("ir")
                self.put(2 * rows, self.mine(left, 0, rows))
                self.start("il")
            else:
                self.start("s1a", "s1b")
                self.put(rows + half, self.mine(right, half, rows))
                self.start("ownb")
                self.put(2 * rows, self.mine(left, 0, half))
                self.start("owna")
        elif n == 2:
            self.wait("s1a")
            self.put(rows, self.mine(right, 0, half) + self.got(0, half))
            self.start("reda")
            self.wait("s1b")
            self.put(2 * rows + half, self.mine(left, half, rows) + self.got(half, rows))
            self.start("redb")
        elif n == 3:
            total = self.mine(0, 0, rows)
            if self.direct:
                self.wait("ir", "il", "io")
                total = total + self.got(rows, 2 * rows) + self.got(2 * rows, 3 * rows) + self.got(0, rows)
            else:
                self.wait("ownb", "owna", "reda", "redb")
                total = total + self.got(rows, 2 * rows) + self.got(2 * rows, 3 * rows)
            self.full[pl.ds(self.row(0), rows), :] = self.finish(total)
            if self.direct:
                self.start("go")
            self.start("gr", "gl", "gp")
        elif n == 4:
            self.wait("gr")
            if not self.direct:
                self.start("fa")
            self.start("flp")
            self.wait("gl")
            if not self.direct:
                self.start("fb")
            self.start("frp")
        elif n == 5:
            if self.direct:
                self.wait("go")
            else:
                self.wait("fa", "fb")
            self.start("fop")
        elif n == 6:
            self.wait("gp", "flp", "frp", "fop")

    def drain(self):
        for kind in self.kinds:
            self.copy(kind).wait_send()


def kernel(cfg, theta_hbm, lam_ref, mu_ref, ut_ref, a_hbm, y_ref, th_out, sb_out, kb_out, kv_out, th, tb, av, sa, sb, kb, kv,
           load_sem, store_sem, *chunk_bufs):
    chips, band, step, lik = cfg
    n_part, dim = th.shape
    m_rows = av.shape[0]
    nb, mc = n_part // 2, m_rows // 2
    owners = CORES * chips
    own = nb // owners
    wide, sub = dim // 2, 512
    rank = ut_ref.shape[0]
    pull = 2.0 / band
    gain = step / n_part
    me = lax.axis_index("feat")
    core, chip = lax.rem(me, CORES), me // CORES
    group = lax.axis_index("ens") * owners
    chip_of = {hop: lax.rem(chip + hop + chips, chips) for hop in (-1, 0, 1, 2)}
    ids = {hop: group + chip_of[hop] * CORES + core for hop in (-1, 1, 2)}
    ids["pair"] = group + chip * CORES + (1 - core)
    where = (core, chip, chips, chip_of, ids)

    def finish(name):
        if name[0] == "g":
            return lambda g: g
        lo = 0 if name in ("z0", "z1") else mc

        def residual(z):
            return (y_ref[:, lo:lo + mc].astype(F32) - 1.0 / (1.0 + jnp.exp(-z))).astype(BF16)
        return residual

    ch = {}
    for k, name in enumerate(CHUNKS):
        ch[name] = Chunk(name, chunk_bufs[7 * k:7 * k + 7], where, finish(name))

    def rows(i):
        return slice(i * nb, (i + 1) * nb)

    def load_theta(i):
        return pltpu.make_async_copy(theta_hbm.at[pl.ds(i * nb, nb), :], th.at[pl.ds(i * nb, nb), :], load_sem.at[i])

    def load_a(j):
        return pltpu.make_async_copy(a_hbm.at[pl.ds(j * mc, mc), :], av.at[pl.ds(j * mc, mc), :], load_sem.at[2 + j])

    load_theta(0).start()
    load_a(0).start()
    load_a(1).start()
    load_theta(1).start()

    barrier = pltpu.get_barrier_semaphore()
    for peer in ids.values():
        pl.semaphore_signal(barrier, inc=1, device_id=peer, device_id_type=LOGICAL)
    pl.semaphore_wait(barrier, len(ids))

    def columns(lo, hi):
        return [slice(n, n + sub) for n in range(lo, hi, sub)]

    def prep(i):
        load_theta(i).wait()

        @pl.loop(0, dim // wide)
        def _(t):
            n = pl.ds(pl.multiple_of(t * wide, wide), wide)
            tb[rows(i), n] = th[rows(i), n].astype(BF16)

    def project():
        q = jnp.zeros((rank, n_part), F32)
        for n in columns(0, dim):
            q = q + dot(ut_ref[:, n], (th[:, n] - mu_ref[:, n]).astype(BF16), NT)
        piece, part = 2 * own + 8, rank // owners
        for o in range(owners):
            for i in range(2):
                lo = o * piece + 2 * own + i * part
                ch["g1"].part[lo:lo + part, :] = q[o * part:(o + 1) * part, rows(i)]

    def gram(i):
        g = dot(tb[rows(i), :], tb[0:(i + 1) * nb, :], NT)
        part = ch[f"g{i}"].part
        piece = part.shape[0] // owners
        for j in range(i + 1):
            for o in range(owners):
                part[o * piece + j * own:o * piece + (j + 1) * own, :] = g[o * own:(o + 1) * own, j * nb:(j + 1) * nb]

    def logit(name, i, j):
        ch[name].part[...] = dot(tb[rows(i), :], av[j * mc:(j + 1) * mc, :], NT)

    def base(i, n, q):
        x = th[rows(i), n] - mu_ref[:, n]
        return x * lam_ref[:, n] + dot(q, ut_ref[:, n]) + pull * tb[rows(i), n].astype(F32)

    def gathered_q(i):
        piece, part = 2 * own + 8, rank // owners
        los = [o * piece + 2 * own + i * part for o in range(owners)]
        return jnp.concatenate([ch["g1"].full[lo:lo + part, :] for lo in los], axis=0).T.astype(BF16)

    def both_lik(lo, hi):
        for n in columns(lo, hi):
            sa[rows(0), n] = lik * (dot(ch["z0"].full[...], av[0:mc, n]) + dot(ch["z3"].full[...], av[mc:2 * mc, n]))

    def first_lik(lo, hi):
        for n in columns(lo, hi):
            sa[rows(1), n] = lik * dot(ch["z1"].full[...], av[0:mc, n])

    def last_lik(lo, hi):
        for n in columns(lo, hi):
            sb[rows(1), n] = (sa[rows(1), n] + lik * dot(ch["z2"].full[...], av[mc:2 * mc, n])).astype(BF16)

    def low_rank(i):
        q = gathered_q(i)
        for n in columns(0, dim):
            s = sa[rows(i), n] - base(i, n, q)
            if i == 0:
                sb[rows(i), n] = s.astype(BF16)
            else:
                sa[rows(i), n] = s

    def kernel_mat():
        def block(name, j):
            full = ch[name].full
            piece = full.shape[0] // owners
            return jnp.concatenate(
                [full[o * piece + j * own:o * piece + (j + 1) * own, :] for o in range(owners)], axis=0)

        def diag(g):
            eye = lax.broadcasted_iota(jnp.int32, g.shape, 0) == lax.broadcasted_iota(jnp.int32, g.shape, 1)
            d = jnp.where(eye, g, 0.0)
            return jnp.sum(d, axis=1, keepdims=True), jnp.sum(d, axis=0, keepdims=True)

        def rbf(c, r, g):
            return jnp.exp(-jnp.maximum(c + r - 2.0 * g, 0.0) / band)

        g00, g10, g11 = block("g0", 0), block("g1", 0), block("g1", 1)
        (c0, r0), (c1, r1) = diag(g00), diag(g11)
        k00, k10, k11 = rbf(c0, r0, g00), rbf(c1, r0, g10), rbf(c1, r1, g11)
        k01 = k10.T
        for i, j, k in ((0, 0, k00), (0, 1, k01), (1, 0, k10), (1, 1, k11)):
            kb[rows(i), rows(j)] = k.astype(BF16)
        for i, pair in ((0, (k00, k01)), (1, (k10, k11))):
            total = jnp.sum(pair[0], axis=1, keepdims=True) + jnp.sum(pair[1], axis=1, keepdims=True)
            kv[rows(i), :] = jnp.broadcast_to(gain * pull * total, (nb, LANES))

    def drive(i, lo, hi):
        for n in columns(lo, hi):
            t = th[rows(i), n]
            scale = jnp.concatenate([kv[rows(i), :]] * (sub // LANES), axis=1)
            t = t + (scale * t + gain * dot(kb[rows(i), :], sb[:, n]))
            th[rows(i), n] = t
            tb[rows(i), n] = t.astype(BF16)

    outs = dict(th0=(th, th_out, rows(0)), th1=(th, th_out, rows(1)), sb0=(sb, sb_out, rows(0)),
                sb1=(sb, sb_out, rows(1)), kb=(kb, kb_out, slice(0, n_part)), kv=(kv, kv_out, slice(0, n_part)))
    out_copies = {}
    for k, (name, (src, dst, r)) in enumerate(outs.items()):
        out_copies[name] = pltpu.make_async_copy(src.at[r, :], dst.at[r, :], store_sem.at[k])
    ready = {"drive1b": ("th0", "th1"), "lr0": ("sb0",), "ll1b": ("sb1",), "kmat": ("kb", "kv")}

    halves = {"a": (0, wide), "b": (wide, dim)}
    pieces = {
        "proj": project, "gram0": lambda: gram(0), "gram1": lambda: gram(1),
        "z0p": lambda: logit("z0", 0, 0), "z0q": lambda: logit("z3", 0, 1),
        "z1": lambda: logit("z1", 1, 0), "z2": lambda: logit("z2", 1, 1),
        "lr0": lambda: low_rank(0), "lr1": lambda: low_rank(1), "kmat": kernel_mat,
    }
    for h, (lo, hi) in halves.items():
        pieces["l0" + h] = functools.partial(both_lik, lo, hi)
        pieces["lf1" + h] = functools.partial(first_lik, lo, hi)
        pieces["ll1" + h] = functools.partial(last_lik, lo, hi)
        pieces["drive0" + h] = functools.partial(drive, 0, lo, hi)
        pieces["drive1" + h] = functools.partial(drive, 1, lo, hi)

    @pl.loop(0, NUM_STEPS)
    def _(s):
        @pl.when(s == 0)
        def _():
            prep(0)

        loaded = set()
        for item in SCHEDULE:
            if ":" in item:
                name, n = item.split(":")
                ch[name].stage(int(n))
                continue
            if item in ("z0p", "z0q"):
                @pl.when(s == 0)
                def _():
                    load_a("pq".index(item[-1])).wait()
            if item == "drive1a":
                @pl.when(s == 0)
                def _():
                    prep(1)
            if item[:6] == "drive1":
                pl.when(s > 0)(pieces[item])
            elif item[:6] == "drive0":
                pl.when(s < NUM_STEPS - 1)(pieces[item])
            else:
                pieces[item]()
            if item in ready:
                @pl.when(s == NUM_STEPS - 1)
                def _():
                    for name in ready[item]:
                        out_copies[name].start()
        for name in CHUNKS:
            ch[name].drain()

    for copy in out_copies.values():
        copy.wait()


def last_drive(gain, th_ref, sb_ref, kb_ref, kv_ref, out_ref):
    t = th_ref[...]
    scale = jnp.concatenate([kv_ref[...]] * (t.shape[1] // LANES), axis=1)
    out_ref[...] = t + (scale * t + gain * dot(kb_ref[...], sb_ref[...]))


def solution(mesh):
    feat_size = mesh.shape["feat"]
    chips = feat_size // CORES

    def local_run(particles, prec_diag, low_factor, prior_mean, data_mat, labels):
        n_part, dim = particles.shape
        m_rows = data_mat.shape[0]
        dim_full = dim * feat_size
        cfg = (chips, 2.0 * dim_full, dim_full / 4.0, 2.0 / math.sqrt(m_rows * dim_full))
        nb, mc = n_part // 2, m_rows // 2
        own = nb // feat_size
        vm, any_ = pl.BlockSpec(memory_space=pltpu.VMEM), pl.BlockSpec(memory_space=pl.ANY)
        dma = pltpu.SemaphoreType.DMA
        scratch = [
            pltpu.VMEM((n_part, dim), F32), pltpu.VMEM((n_part, dim), BF16), pltpu.VMEM((m_rows, dim), BF16),
            pltpu.VMEM((n_part, dim), F32), pltpu.VMEM((n_part, dim), BF16),
            pltpu.VMEM((n_part, n_part), BF16), pltpu.VMEM((n_part, LANES), F32), dma((4,)), dma((6,)),
        ]
        for name in CHUNKS:
            wire, width, rows = (F32, nb, own) if name[0] == "g" else (BF16, mc, own)
            if name == "g1":
                rows = 2 * own + 8
            count = len(DIRECT_KINDS if name in DIRECT else KINDS)
            scratch += [
                pltpu.VMEM((feat_size * rows, width), F32), pltpu.VMEM((chips * rows, width), F32),
                pltpu.VMEM((3 * rows, width), wire), pltpu.VMEM((3 * rows, width), wire),
                pltpu.VMEM((feat_size * rows, width), wire), dma((count,)), dma((count,)),
            ]
        outs = [((n_part, dim), F32), ((n_part, dim), BF16), ((n_part, n_part), BF16), ((n_part, LANES), F32)]
        th, sb, kb, kv = pl.pallas_call(
            functools.partial(kernel, cfg),
            out_shape=[jax.ShapeDtypeStruct(*o) for o in outs],
            in_specs=[any_, vm, vm, vm, any_, vm],
            out_specs=[any_] * 4,
            scratch_shapes=scratch,
            compiler_params=pltpu.CompilerParams(
                collective_id=0, has_side_effects=True, vmem_limit_bytes=60 * 2**20),
            cost_estimate=pl.CostEstimate(flops=60 * 10**9, bytes_accessed=32 * 2**20, transcendentals=0),
        )(particles, prec_diag[None, :], prior_mean[None, :], low_factor.T, data_mat, labels[None, :])
        width = 512
        by_column = pl.BlockSpec((n_part, width), lambda n: (0, n))
        whole = lambda x: pl.BlockSpec(x.shape, lambda n: (0, 0))
        return pl.pallas_call(
            functools.partial(last_drive, dim_full / 4.0 / n_part),
            out_shape=jax.ShapeDtypeStruct((n_part, dim), F32),
            grid=(dim // width,),
            in_specs=[by_column, by_column, whole(kb), whole(kv)],
            out_specs=by_column,
            cost_estimate=pl.CostEstimate(flops=2 * n_part * n_part * dim, bytes_accessed=20 * 2**20, transcendentals=0),
        )(th, sb, kb, kv)

    return jax.shard_map(
        local_run,
        mesh=mesh,
        in_specs=(P("ens", "feat"), P(("ens", "feat")), P(("ens", "feat"), None),
                  P(("ens", "feat")), P("ens", "feat"), P("ens")),
        out_specs=P("ens", "feat"),
        check_vma=False,
    )
```

```python
import functools
import math
import jax
import jax.numpy as jnp
from jax import lax
from jax.experimental import pallas as pl
from jax.experimental.pallas import tpu as pltpu
from jax.sharding import PartitionSpec as P

NUM_STEPS = 3
CORES = 2
LANES = 128
F32, BF16 = jnp.float32, jnp.bfloat16
NN = (((1,), (0,)), ((), ()))
NT = (((1,), (1,)), ((), ()))
LOGICAL = pl.DeviceIdType.LOGICAL
KINDS = ("d2d", "s1a", "s1b", "ownb", "owna", "reda", "redb",
         "gr", "gl", "gp", "fa", "flp", "fb", "frp", "fop")
DIRECT_KINDS = ("d2d", "ir", "il", "io", "gr", "gl", "go", "gp", "flp", "frp", "fop")
CHUNKS = ("g0", "z0", "z3", "g1", "z1", "z2")
DIRECT = ('g0', 'g1', 'z0', 'z1', 'z2', 'z3')
SCHEDULE = (
    "z0q", "z3:0", "z0p", "z0:0", "z3:1", "gram0", "z0:1", "g0:0", "drive1a", "drive1b", "g0:1", "z1",
    "z3:3", "z1:0", "gram1", "z0:3", "proj", "g1:0", "z1:1", "g1:1", "z3:4", "z3:5", "z2", "z0:4",
    "z1:3", "z0:5", "z2:0", "z2:1", "z3:6", "g1:3", "z0:6", "z1:4", "l0a", "z2:3", "g0:3", "z1:5",
    "l0b", "z1:6", "lf1a", "lf1b", "g1:4", "g1:5", "z2:4", "z2:5", "g1:6", "lr1", "z2:6", "ll1a",
    "g0:4", "g0:5", "ll1b", "lr0", "g0:6", "kmat", "drive0a", "drive0b",
)


def dot(a, b, dims=NN):
    return lax.dot_general(a, b, dims, preferred_element_type=F32)


class Chunk:
    def __init__(self, name, bufs, where, finish):
        self.part, self.pair, self.send, self.recv, self.full, self.ssem, self.rsem = bufs
        self.core, self.chip, self.chips, self.chip_of, self.ids = where
        self.rows = self.full.shape[0] // (CORES * self.chips)
        self.half = self.rows // 32 * 16
        self.direct = name in DIRECT
        self.kinds = DIRECT_KINDS if self.direct else KINDS
        self.finish = finish

    def row(self, hop):
        return pl.multiple_of((self.core * self.chips + self.chip_of[hop]) * self.rows, 8)

    def copy(self, kind):
        rows, half = self.rows, self.half
        core, pair = self.core, self.ids["pair"]
        chip, right, left, opp = 0, 1, -1, 2
        at = lambda hop: self.ids[hop]
        snd, rcv, full = self.send, self.recv, self.full

        def same(lo, size):
            ref = full.at[pl.ds(lo, size), :]
            return ref, ref

        def slot(lo, hi):
            return snd.at[pl.ds(lo, hi - lo), :], rcv.at[pl.ds(lo, hi - lo), :]

        if kind == "d2d":
            size = self.chips * rows
            src, dst = self.part.at[pl.ds(pl.multiple_of((1 - core) * size, 8), size), :], self.pair
            dev = pair
        else:
            (src, dst), dev = {
                "s1a": lambda: (slot(0, half), at(right)),
                "s1b": lambda: (slot(half, rows), at(left)),
                "ownb": lambda: (slot(rows + half, 2 * rows), at(right)),
                "owna": lambda: (slot(2 * rows, 2 * rows + half), at(left)),
                "reda": lambda: (slot(rows, rows + half), at(right)),
                "redb": lambda: (slot(2 * rows + half, 3 * rows), at(left)),
                "io": lambda: (slot(0, rows), at(opp)),
                "ir": lambda: (slot(rows, 2 * rows), at(right)),
                "il": lambda: (slot(2 * rows, 3 * rows), at(left)),
                "gr": lambda: (same(self.row(chip), rows), at(right)),
                "gl": lambda: (same(self.row(chip), rows), at(left)),
                "go": lambda: (same(self.row(chip), rows), at(opp)),
                "gp": lambda: (same(self.row(chip), rows), pair),
                "fa": lambda: (same(self.row(left), half), at(right)),
                "flp": lambda: (same(self.row(left), rows), pair),
                "fb": lambda: (same(self.row(right) + half, rows - half), at(left)),
                "frp": lambda: (same(self.row(right), rows), pair),
                "fop": lambda: (same(self.row(opp), rows), pair),
            }[kind]()
        k = self.kinds.index(kind)
        return pltpu.make_async_remote_copy(
            src_ref=src, dst_ref=dst, send_sem=self.ssem.at[k], recv_sem=self.rsem.at[k],
            device_id=dev, device_id_type=LOGICAL)

    def start(self, *kinds):
        for kind in kinds:
            self.copy(kind).start()

    def wait(self, *kinds):
        for kind in kinds:
            self.copy(kind).wait_recv()

    def mine(self, hop, lo, hi):
        a = self.part[pl.ds(self.row(hop) + lo, hi - lo), :]
        b = self.pair[pl.ds(pl.multiple_of(self.chip_of[hop] * self.rows, 8) + lo, hi - lo), :]
        return a + b

    def put(self, lo, value):
        self.send[lo:lo + value.shape[0], :] = value.astype(self.send.dtype)

    def got(self, lo, hi):
        return self.recv[lo:hi, :].astype(F32)

    def stage(self, n):
        rows, half = self.rows, self.half
        right, left, opp = 1, -1, 2
        if n == 0:
            self.start("d2d")
        elif n == 1:
            self.wait("d2d")
            self.put(0, self.mine(opp, 0, rows))
            if self.direct:
                self.start("io")
                self.put(rows, self.mine(right, 0, rows))
                self.start("ir")
                self.put(2 * rows, self.mine(left, 0, rows))
                self.start("il")
            else:
                self.start("s1a", "s1b")
                self.put(rows + half, self.mine(right, half, rows))
                self.start("ownb")
                self.put(2 * rows, self.mine(left, 0, half))
                self.start("owna")
        elif n == 2:
            self.wait("s1a")
            self.put(rows, self.mine(right, 0, half) + self.got(0, half))
            self.start("reda")
            self.wait("s1b")
            self.put(2 * rows + half, self.mine(left, half, rows) + self.got(half, rows))
            self.start("redb")
        elif n == 3:
            total = self.mine(0, 0, rows)
            if self.direct:
                self.wait("ir", "il", "io")
                total = total + self.got(rows, 2 * rows) + self.got(2 * rows, 3 * rows) + self.got(0, rows)
            else:
                self.wait("ownb", "owna", "reda", "redb")
                total = total + self.got(rows, 2 * rows) + self.got(2 * rows, 3 * rows)
            self.full[pl.ds(self.row(0), rows), :] = self.finish(total)
            if self.direct:
                self.start("go")
            self.start("gr", "gl", "gp")
        elif n == 4:
            self.wait("gr")
            if not self.direct:
                self.start("fa")
            self.start("flp")
            self.wait("gl")
            if not self.direct:
                self.start("fb")
            self.start("frp")
        elif n == 5:
            if self.direct:
                self.wait("go")
            else:
                self.wait("fa", "fb")
            self.start("fop")
        elif n == 6:
            self.wait("gp", "flp", "frp", "fop")

    def drain(self):
        for kind in self.kinds:
            self.copy(kind).wait_send()


def kernel(cfg, theta_hbm, lam_ref, mu_ref, ut_ref, a_hbm, y_ref, th, tb, av, sa, sb, kb, kv,
           load_sem, *chunk_bufs):
    chips, band, step, lik = cfg
    n_part, dim = th.shape
    m_rows = av.shape[0]
    nb, mc = n_part // 2, m_rows // 2
    owners = CORES * chips
    own = nb // owners
    wide, sub = dim // 2, 512
    rank = ut_ref.shape[0]
    pull = 2.0 / band
    gain = step / n_part
    me = lax.axis_index("feat")
    core, chip = lax.rem(me, CORES), me // CORES
    group = lax.axis_index("ens") * owners
    chip_of = {hop: lax.rem(chip + hop + chips, chips) for hop in (-1, 0, 1, 2)}
    ids = {hop: group + chip_of[hop] * CORES + core for hop in (-1, 1, 2)}
    ids["pair"] = group + chip * CORES + (1 - core)
    where = (core, chip, chips, chip_of, ids)

    def finish(name):
        if name[0] == "g":
            return lambda g: g
        lo = 0 if name in ("z0", "z1") else mc

        def residual(z):
            return (y_ref[:, lo:lo + mc].astype(F32) - 1.0 / (1.0 + jnp.exp(-z))).astype(BF16)
        return residual

    ch = {}
    for k, name in enumerate(CHUNKS):
        ch[name] = Chunk(name, chunk_bufs[7 * k:7 * k + 7], where, finish(name))

    def rows(i):
        return slice(i * nb, (i + 1) * nb)

    def load_theta(i):
        return pltpu.make_async_copy(theta_hbm.at[pl.ds(i * nb, nb), :], th.at[pl.ds(i * nb, nb), :], load_sem.at[i])

    def load_a(j):
        return pltpu.make_async_copy(a_hbm.at[pl.ds(j * mc, mc), :], av.at[pl.ds(j * mc, mc), :], load_sem.at[2 + j])

    load_theta(0).start()
    load_a(0).start()
    load_a(1).start()
    load_theta(1).start()

    barrier = pltpu.get_barrier_semaphore()
    for peer in ids.values():
        pl.semaphore_signal(barrier, inc=1, device_id=peer, device_id_type=LOGICAL)
    pl.semaphore_wait(barrier, len(ids))

    def columns(lo, hi):
        return [slice(n, n + sub) for n in range(lo, hi, sub)]

    def prep(i):
        load_theta(i).wait()

        @pl.loop(0, dim // wide)
        def _(t):
            n = pl.ds(pl.multiple_of(t * wide, wide), wide)
            tb[rows(i), n] = th[rows(i), n].astype(BF16)

    def project():
        q = jnp.zeros((rank, n_part), F32)
        for n in columns(0, dim):
            q = q + dot(ut_ref[:, n], (th[:, n] - mu_ref[:, n]).astype(BF16), NT)
        piece, part = 2 * own + 8, rank // owners
        for o in range(owners):
            for i in range(2):
                lo = o * piece + 2 * own + i * part
                ch["g1"].part[lo:lo + part, :] = q[o * part:(o + 1) * part, rows(i)]

    def gram(i):
        g = dot(tb[rows(i), :], tb[0:(i + 1) * nb, :], NT)
        part = ch[f"g{i}"].part
        piece = part.shape[0] // owners
        for j in range(i + 1):
            for o in range(owners):
                part[o * piece + j * own:o * piece + (j + 1) * own, :] = g[o * own:(o + 1) * own, j * nb:(j + 1) * nb]

    def logit(name, i, j):
        ch[name].part[...] = dot(tb[rows(i), :], av[j * mc:(j + 1) * mc, :], NT)

    def base(i, n, q):
        x = th[rows(i), n] - mu_ref[:, n]
        return x * lam_ref[:, n] + dot(q, ut_ref[:, n]) + pull * tb[rows(i), n].astype(F32)

    def gathered_q(i):
        piece, part = 2 * own + 8, rank // owners
        los = [o * piece + 2 * own + i * part for o in range(owners)]
        return jnp.concatenate([ch["g1"].full[lo:lo + part, :] for lo in los], axis=0).T.astype(BF16)

    def both_lik(lo, hi):
        for n in columns(lo, hi):
            sa[rows(0), n] = lik * (dot(ch["z0"].full[...], av[0:mc, n]) + dot(ch["z3"].full[...], av[mc:2 * mc, n]))

    def first_lik(lo, hi):
        for n in columns(lo, hi):
            sa[rows(1), n] = lik * dot(ch["z1"].full[...], av[0:mc, n])

    def last_lik(lo, hi):
        for n in columns(lo, hi):
            sb[rows(1), n] = (sa[rows(1), n] + lik * dot(ch["z2"].full[...], av[mc:2 * mc, n])).astype(BF16)

    def low_rank(i):
        q = gathered_q(i)
        for n in columns(0, dim):
            s = sa[rows(i), n] - base(i, n, q)
            if i == 0:
                sb[rows(i), n] = s.astype(BF16)
            else:
                sa[rows(i), n] = s

    def kernel_mat():
        def block(name, j):
            full = ch[name].full
            piece = full.shape[0] // owners
            return jnp.concatenate(
                [full[o * piece + j * own:o * piece + (j + 1) * own, :] for o in range(owners)], axis=0)

        def diag(g):
            eye = lax.broadcasted_iota(jnp.int32, g.shape, 0) == lax.broadcasted_iota(jnp.int32, g.shape, 1)
            d = jnp.where(eye, g, 0.0)
            return jnp.sum(d, axis=1, keepdims=True), jnp.sum(d, axis=0, keepdims=True)

        def rbf(c, r, g):
            return jnp.exp(-jnp.maximum(c + r - 2.0 * g, 0.0) / band)

        g00, g10, g11 = block("g0", 0), block("g1", 0), block("g1", 1)
        (c0, r0), (c1, r1) = diag(g00), diag(g11)
        k00, k10, k11 = rbf(c0, r0, g00), rbf(c1, r0, g10), rbf(c1, r1, g11)
        k01 = k10.T
        for i, j, k in ((0, 0, k00), (0, 1, k01), (1, 0, k10), (1, 1, k11)):
            kb[rows(i), rows(j)] = k.astype(BF16)
        for i, pair in ((0, (k00, k01)), (1, (k10, k11))):
            total = jnp.sum(pair[0], axis=1, keepdims=True) + jnp.sum(pair[1], axis=1, keepdims=True)
            kv[rows(i), :] = jnp.broadcast_to(gain * pull * total, (nb, LANES))

    def drive(i, lo, hi):
        for n in columns(lo, hi):
            t = th[rows(i), n]
            scale = jnp.concatenate([kv[rows(i), :]] * (sub // LANES), axis=1)
            t = t + (scale * t + gain * dot(kb[rows(i), :], sb[:, n]))
            th[rows(i), n] = t
            tb[rows(i), n] = t.astype(BF16)

    halves = {"a": (0, wide), "b": (wide, dim)}
    pieces = {
        "proj": project, "gram0": lambda: gram(0), "gram1": lambda: gram(1),
        "z0p": lambda: logit("z0", 0, 0), "z0q": lambda: logit("z3", 0, 1),
        "z1": lambda: logit("z1", 1, 0), "z2": lambda: logit("z2", 1, 1),
        "lr0": lambda: low_rank(0), "lr1": lambda: low_rank(1), "kmat": kernel_mat,
    }
    for h, (lo, hi) in halves.items():
        pieces["l0" + h] = functools.partial(both_lik, lo, hi)
        pieces["lf1" + h] = functools.partial(first_lik, lo, hi)
        pieces["ll1" + h] = functools.partial(last_lik, lo, hi)
        pieces["drive0" + h] = functools.partial(drive, 0, lo, hi)
        pieces["drive1" + h] = functools.partial(drive, 1, lo, hi)

    @pl.loop(0, NUM_STEPS)
    def _(s):
        @pl.when(s == 0)
        def _():
            prep(0)

        loaded = set()
        for item in SCHEDULE:
            if ":" in item:
                name, n = item.split(":")
                ch[name].stage(int(n))
                continue
            if item in ("z0p", "z0q"):
                @pl.when(s == 0)
                def _():
                    load_a("pq".index(item[-1])).wait()
            if item == "drive1a":
                @pl.when(s == 0)
                def _():
                    prep(1)
            if item[:6] == "drive1":
                pl.when(s > 0)(pieces[item])
            else:
                pieces[item]()
        for name in CHUNKS:
            ch[name].drain()

    for lo, hi in halves.values():
        drive(1, lo, hi)


def solution(mesh):
    feat_size = mesh.shape["feat"]
    chips = feat_size // CORES

    def local_run(particles, prec_diag, low_factor, prior_mean, data_mat, labels):
        n_part, dim = particles.shape
        m_rows = data_mat.shape[0]
        dim_full = dim * feat_size
        cfg = (chips, 2.0 * dim_full, dim_full / 4.0, 2.0 / math.sqrt(m_rows * dim_full))
        nb, mc = n_part // 2, m_rows // 2
        own = nb // feat_size
        vm, any_ = pl.BlockSpec(memory_space=pltpu.VMEM), pl.BlockSpec(memory_space=pl.ANY)
        dma = pltpu.SemaphoreType.DMA
        scratch = [
            pltpu.VMEM((n_part, dim), BF16), pltpu.VMEM((m_rows, dim), BF16),
            pltpu.VMEM((n_part, dim), F32), pltpu.VMEM((n_part, dim), BF16),
            pltpu.VMEM((n_part, n_part), BF16), pltpu.VMEM((n_part, LANES), F32), dma((4,)),
        ]
        for name in CHUNKS:
            wire, width, rows = (F32, nb, own) if name[0] == "g" else (BF16, mc, own)
            if name == "g1":
                rows = 2 * own + 8
            count = len(DIRECT_KINDS if name in DIRECT else KINDS)
            scratch += [
                pltpu.VMEM((feat_size * rows, width), F32), pltpu.VMEM((chips * rows, width), F32),
                pltpu.VMEM((3 * rows, width), wire), pltpu.VMEM((3 * rows, width), wire),
                pltpu.VMEM((feat_size * rows, width), wire), dma((count,)), dma((count,)),
            ]
        return pl.pallas_call(
            functools.partial(kernel, cfg),
            out_shape=pltpu.VMEM((n_part, dim), F32),
            in_specs=[any_, vm, vm, vm, any_, vm],
            out_specs=vm,
            scratch_shapes=scratch,
            compiler_params=pltpu.CompilerParams(
                collective_id=0, has_side_effects=True, vmem_limit_bytes=48 * 2**20),
            cost_estimate=pl.CostEstimate(flops=60 * 10**9, bytes_accessed=32 * 2**20, transcendentals=0),
        )(particles, prec_diag[None, :], prior_mean[None, :], low_factor.T, data_mat, labels[None, :])

    return jax.shard_map(
        local_run,
        mesh=mesh,
        in_specs=(P("ens", "feat"), P(("ens", "feat")), P(("ens", "feat"), None),
                  P(("ens", "feat")), P("ens", "feat"), P("ens")),
        out_specs=P("ens", "feat"),
        check_vma=False,
    )
```

```python
import functools
import math
import jax
import jax.numpy as jnp
from jax import lax
from jax.experimental import pallas as pl
from jax.experimental.pallas import tpu as pltpu
from jax.sharding import PartitionSpec as P

NUM_STEPS = 3
CORES = 2
LANES = 128
F32, BF16 = jnp.float32, jnp.bfloat16
NN = (((1,), (0,)), ((), ()))
NT = (((1,), (1,)), ((), ()))
LOGICAL = pl.DeviceIdType.LOGICAL
KINDS = ("d2d", "s1a", "s1b", "ownb", "owna", "reda", "redb",
         "gr", "gl", "gp", "fa", "flp", "fb", "frp", "fop")
DIRECT_KINDS = ("d2d", "ir", "il", "io", "gr", "gl", "go", "gp", "flp", "frp", "fop")
CHUNKS = ("g0", "z0", "z3", "g1", "z1", "z2")
DIRECT = ('z0', 'z3', 'z1', 'z2', 'g0', 'g1')
SCHEDULE = (
    "gram0", "g0:0", "z0p", "z0:0", "drive1a", "g0:1", "z0q", "z3:0", "drive1b", "z0:1", "z1", "z1:0",
    "z3:1", "proj", "z1:1", "gram1", "z0:3", "g1:0", "z3:3", "z2", "z2:0", "g1:1", "z1:3", "z2:1",
    "z3:4", "z3:5", "z0:4", "z0:5", "g1:3", "z1:4", "z3:6", "z0:6", "z1:5", "l0a", "g0:3", "z1:6",
    "z2:3", "lf1a", "lf1b", "l0b", "g1:4", "g1:5", "g0:4", "g0:5", "g1:6", "lr0", "z2:4", "z2:5",
    "lr1", "g0:6", "kmat", "z2:6", "ll1a", "d1", "d0", "ll1b", "drive0a", "drive0b",
)


def dot(a, b, dims=NN):
    return lax.dot_general(a, b, dims, preferred_element_type=F32)


class Chunk:
    def __init__(self, name, bufs, where, finish):
        self.part, self.pair, self.send, self.recv, self.full, self.ssem, self.rsem = bufs
        self.core, self.chip, self.chips, self.chip_of, self.ids = where
        self.rows = self.full.shape[0] // (CORES * self.chips)
        self.half = self.rows // 32 * 16
        self.direct = name in DIRECT
        self.kinds = DIRECT_KINDS if self.direct else KINDS
        self.finish = finish

    def row(self, hop):
        return pl.multiple_of((self.core * self.chips + self.chip_of[hop]) * self.rows, 8)

    def copy(self, kind):
        rows, half = self.rows, self.half
        core, pair = self.core, self.ids["pair"]
        chip, right, left, opp = 0, 1, -1, 2
        at = lambda hop: self.ids[hop]
        snd, rcv, full = self.send, self.recv, self.full

        def same(lo, size):
            ref = full.at[pl.ds(lo, size), :]
            return ref, ref

        def slot(lo, hi):
            return snd.at[pl.ds(lo, hi - lo), :], rcv.at[pl.ds(lo, hi - lo), :]

        if kind == "d2d":
            size = self.chips * rows
            src, dst = self.part.at[pl.ds(pl.multiple_of((1 - core) * size, 8), size), :], self.pair
            dev = pair
        else:
            (src, dst), dev = {
                "s1a": lambda: (slot(0, half), at(right)),
                "s1b": lambda: (slot(half, rows), at(left)),
                "ownb": lambda: (slot(rows + half, 2 * rows), at(right)),
                "owna": lambda: (slot(2 * rows, 2 * rows + half), at(left)),
                "reda": lambda: (slot(rows, rows + half), at(right)),
                "redb": lambda: (slot(2 * rows + half, 3 * rows), at(left)),
                "io": lambda: (slot(0, rows), at(opp)),
                "ir": lambda: (slot(rows, 2 * rows), at(right)),
                "il": lambda: (slot(2 * rows, 3 * rows), at(left)),
                "gr": lambda: (same(self.row(chip), rows), at(right)),
                "gl": lambda: (same(self.row(chip), rows), at(left)),
                "go": lambda: (same(self.row(chip), rows), at(opp)),
                "gp": lambda: (same(self.row(chip), rows), pair),
                "fa": lambda: (same(self.row(left), half), at(right)),
                "flp": lambda: (same(self.row(left), rows), pair),
                "fb": lambda: (same(self.row(right) + half, rows - half), at(left)),
                "frp": lambda: (same(self.row(right), rows), pair),
                "fop": lambda: (same(self.row(opp), rows), pair),
            }[kind]()
        k = self.kinds.index(kind)
        return pltpu.make_async_remote_copy(
            src_ref=src, dst_ref=dst, send_sem=self.ssem.at[k], recv_sem=self.rsem.at[k],
            device_id=dev, device_id_type=LOGICAL)

    def start(self, *kinds):
        for kind in kinds:
            self.copy(kind).start()

    def wait(self, *kinds):
        for kind in kinds:
            self.copy(kind).wait_recv()

    def mine(self, hop, lo, hi):
        a = self.part[pl.ds(self.row(hop) + lo, hi - lo), :]
        b = self.pair[pl.ds(pl.multiple_of(self.chip_of[hop] * self.rows, 8) + lo, hi - lo), :]
        return a + b

    def put(self, lo, value):
        self.send[lo:lo + value.shape[0], :] = value.astype(self.send.dtype)

    def got(self, lo, hi):
        return self.recv[lo:hi, :].astype(F32)

    def stage(self, n):
        rows, half = self.rows, self.half
        right, left, opp = 1, -1, 2
        if n == 0:
            self.start("d2d")
        elif n == 1:
            self.wait("d2d")
            self.put(0, self.mine(opp, 0, rows))
            if self.direct:
                self.start("io")
                self.put(rows, self.mine(right, 0, rows))
                self.start("ir")
                self.put(2 * rows, self.mine(left, 0, rows))
                self.start("il")
            else:
                self.start("s1a", "s1b")
                self.put(rows + half, self.mine(right, half, rows))
                self.start("ownb")
                self.put(2 * rows, self.mine(left, 0, half))
                self.start("owna")
        elif n == 2:
            self.wait("s1a")
            self.put(rows, self.mine(right, 0, half) + self.got(0, half))
            self.start("reda")
            self.wait("s1b")
            self.put(2 * rows + half, self.mine(left, half, rows) + self.got(half, rows))
            self.start("redb")
        elif n == 3:
            total = self.mine(0, 0, rows)
            if self.direct:
                self.wait("ir", "il", "io")
                total = total + self.got(rows, 2 * rows) + self.got(2 * rows, 3 * rows) + self.got(0, rows)
            else:
                self.wait("ownb", "owna", "reda", "redb")
                total = total + self.got(rows, 2 * rows) + self.got(2 * rows, 3 * rows)
            self.full[pl.ds(self.row(0), rows), :] = self.finish(total)
            if self.direct:
                self.start("go")
            self.start("gr", "gl", "gp")
        elif n == 4:
            self.wait("gr")
            if not self.direct:
                self.start("fa")
            self.start("flp")
            self.wait("gl")
            if not self.direct:
                self.start("fb")
            self.start("frp")
        elif n == 5:
            if self.direct:
                self.wait("go")
            else:
                self.wait("fa", "fb")
            self.start("fop")
        elif n == 6:
            self.wait("gp", "flp", "frp", "fop")

    def drain(self):
        for kind in self.kinds:
            self.copy(kind).wait_send()


def kernel(cfg, theta_hbm, lam_ref, mu_ref, ut_ref, a_hbm, y_ref, th, tb, av, sa, sb, kb, kv,
           load_sem, *chunk_bufs):
    chips, band, step, lik = cfg
    n_part, dim = th.shape
    m_rows = av.shape[0]
    nb, mc = n_part // 2, m_rows // 2
    owners = CORES * chips
    own = nb // owners
    wide, sub = dim // 2, 512
    blocks = [[(a, b) for a in (2 * i, 2 * i + 1) for b in range(a + 1)] for i in range(2)]
    share = LANES // owners
    q_row = len(blocks[1]) * share
    g1_piece = q_row + ut_ref.shape[0] // owners * (n_part // LANES)
    rank = ut_ref.shape[0]
    pull = 2.0 / band
    gain = step / n_part
    me = lax.axis_index("feat")
    core, chip = lax.rem(me, CORES), me // CORES
    group = lax.axis_index("ens") * owners
    chip_of = {hop: lax.rem(chip + hop + chips, chips) for hop in (-1, 0, 1, 2)}
    ids = {hop: group + chip_of[hop] * CORES + core for hop in (-1, 1, 2)}
    ids["pair"] = group + chip * CORES + (1 - core)
    where = (core, chip, chips, chip_of, ids)

    def finish(name):
        if name[0] == "g":
            return lambda g: g
        lo = 0 if name in ("z0", "z1") else mc

        def residual(z):
            return (y_ref[:, lo:lo + mc].astype(F32) - 1.0 / (1.0 + jnp.exp(-z))).astype(BF16)
        return residual

    ch = {}
    for k, name in enumerate(CHUNKS):
        ch[name] = Chunk(name, chunk_bufs[7 * k:7 * k + 7], where, finish(name))

    def rows(i):
        return slice(i * nb, (i + 1) * nb)

    def load_theta(i):
        return pltpu.make_async_copy(theta_hbm.at[pl.ds(i * nb, nb), :], th.at[pl.ds(i * nb, nb), :], load_sem.at[i])

    def load_a(j):
        return pltpu.make_async_copy(a_hbm.at[pl.ds(j * mc, mc), :], av.at[pl.ds(j * mc, mc), :], load_sem.at[2 + j])

    load_theta(0).start()
    load_a(0).start()
    load_a(1).start()
    load_theta(1).start()

    barrier = pltpu.get_barrier_semaphore()
    for peer in ids.values():
        pl.semaphore_signal(barrier, inc=1, device_id=peer, device_id_type=LOGICAL)
    pl.semaphore_wait(barrier, len(ids))

    def columns(lo, hi):
        return [slice(n, n + sub) for n in range(lo, hi, sub)]

    def prep(i):
        load_theta(i).wait()

        @pl.loop(0, dim // wide)
        def _(t):
            n = pl.ds(pl.multiple_of(t * wide, wide), wide)
            tb[rows(i), n] = th[rows(i), n].astype(BF16)

    def project():
        q = jnp.zeros((rank, n_part), F32)
        for n in columns(0, dim):
            q = q + dot(ut_ref[:, n], (th[:, n] - mu_ref[:, n]).astype(BF16), NT)
        part = rank // owners
        for o in range(owners):
            for k in range(n_part // LANES):
                lo = o * g1_piece + q_row + k * part
                ch["g1"].part[lo:lo + part, :] = q[o * part:(o + 1) * part, k * LANES:(k + 1) * LANES]

    def gram(i):
        g = dot(tb[rows(i), :], tb[0:(i + 1) * nb, :], NT)
        part = ch[f"g{i}"].part
        piece = part.shape[0] // owners
        for k, (a, b) in enumerate(blocks[i]):
            block = g[(a - 2 * i) * LANES:(a - 2 * i + 1) * LANES, b * LANES:(b + 1) * LANES]
            for o in range(owners):
                part[o * piece + k * share:o * piece + (k + 1) * share, :] = block[o * share:(o + 1) * share]

    def logit(name, i, j):
        ch[name].part[...] = dot(tb[rows(i), :], av[j * mc:(j + 1) * mc, :], NT)

    def base(i, n, q):
        x = th[rows(i), n] - mu_ref[:, n]
        return x * lam_ref[:, n] + dot(q, ut_ref[:, n]) + pull * tb[rows(i), n].astype(F32)

    def gathered_q(i):
        part = rank // owners
        parts = []
        for k in range(i * nb // LANES, (i + 1) * nb // LANES):
            los = [o * g1_piece + q_row + k * part for o in range(owners)]
            parts.append(jnp.concatenate([ch["g1"].full[lo:lo + part, :] for lo in los], axis=0).T)
        return jnp.concatenate(parts, axis=0).astype(BF16)

    def both_lik(lo, hi):
        for n in columns(lo, hi):
            sa[rows(0), n] = lik * (dot(ch["z0"].full[...], av[0:mc, n]) + dot(ch["z3"].full[...], av[mc:2 * mc, n]))

    def first_lik(lo, hi):
        for n in columns(lo, hi):
            sa[rows(1), n] = lik * dot(ch["z1"].full[...], av[0:mc, n])

    def last_lik(lo, hi):
        for n in columns(lo, hi):
            sb[rows(1), n] = (sa[rows(1), n] + lik * dot(ch["z2"].full[...], av[mc:2 * mc, n])).astype(BF16)

    def low_rank(i):
        q = gathered_q(i)
        for n in columns(0, dim):
            s = sa[rows(i), n] - base(i, n, q)
            if i == 0:
                sb[rows(i), n] = s.astype(BF16)
            else:
                sa[rows(i), n] = s

    def kernel_mat():
        grams = {}
        for i in range(2):
            full = ch[f"g{i}"].full
            piece = full.shape[0] // owners
            for k, ab in enumerate(blocks[i]):
                grams[ab] = jnp.concatenate(
                    [full[o * piece + k * share:o * piece + (k + 1) * share, :] for o in range(owners)], axis=0)
        eye = lax.broadcasted_iota(jnp.int32, (LANES, LANES), 0) == lax.broadcasted_iota(jnp.int32, (LANES, LANES), 1)
        count = n_part // LANES
        norms = [jnp.where(eye, grams[a, a], 0.0) for a in range(count)]
        cols = [jnp.sum(d, axis=1, keepdims=True) for d in norms]
        lines = [jnp.sum(d, axis=0, keepdims=True) for d in norms]
        totals = [0.0] * count
        for (a, b), g in grams.items():
            k = jnp.exp(-jnp.maximum(cols[a] + lines[b] - 2.0 * g, 0.0) / band)
            for i, j, m in ((a, b, k), (b, a, k.T))[:2 if a != b else 1]:
                kb[i * LANES:(i + 1) * LANES, j * LANES:(j + 1) * LANES] = m.astype(BF16)
                totals[i] = totals[i] + jnp.sum(m, axis=1, keepdims=True)
        for a in range(count):
            kv[a * LANES:(a + 1) * LANES, :] = jnp.broadcast_to(gain * pull * totals[a], (LANES, LANES))

    def drive_first(i):
        for n in columns(0, dim):
            t = th[rows(i), n]
            scale = jnp.concatenate([kv[rows(i), :]] * (sub // LANES), axis=1)
            th[rows(i), n] = t + (scale * t + gain * dot(kb[rows(i), rows(0)], sb[rows(0), n]))

    def drive(i, lo, hi):
        for n in columns(lo, hi):
            t = th[rows(i), n] + gain * dot(kb[rows(i), rows(1)], sb[rows(1), n])
            th[rows(i), n] = t
            tb[rows(i), n] = t.astype(BF16)

    halves = {"a": (0, wide), "b": (wide, dim)}
    pieces = {
        "proj": project, "gram0": lambda: gram(0), "gram1": lambda: gram(1),
        "z0p": lambda: logit("z0", 0, 0), "z0q": lambda: logit("z3", 0, 1),
        "z1": lambda: logit("z1", 1, 0), "z2": lambda: logit("z2", 1, 1),
        "lr0": lambda: low_rank(0), "lr1": lambda: low_rank(1), "kmat": kernel_mat,
        "d0": lambda: drive_first(0), "d1": lambda: drive_first(1),
    }
    for h, (lo, hi) in halves.items():
        pieces["l0" + h] = functools.partial(both_lik, lo, hi)
        pieces["lf1" + h] = functools.partial(first_lik, lo, hi)
        pieces["ll1" + h] = functools.partial(last_lik, lo, hi)
        pieces["drive0" + h] = functools.partial(drive, 0, lo, hi)
        pieces["drive1" + h] = functools.partial(drive, 1, lo, hi)

    @pl.loop(0, NUM_STEPS)
    def _(s):
        @pl.when(s == 0)
        def _():
            prep(0)

        loaded = set()
        for item in SCHEDULE:
            if ":" in item:
                name, n = item.split(":")
                ch[name].stage(int(n))
                continue
            if item in ("z0p", "z0q"):
                @pl.when(s == 0)
                def _():
                    load_a("pq".index(item[-1])).wait()
            if item == "drive1a":
                @pl.when(s == 0)
                def _():
                    prep(1)
            if item[:6] == "drive1":
                pl.when(s > 0)(pieces[item])
            else:
                pieces[item]()
        for name in CHUNKS:
            ch[name].drain()

    for lo, hi in halves.values():
        drive(1, lo, hi)


def solution(mesh):
    feat_size = mesh.shape["feat"]
    chips = feat_size // CORES

    def local_run(particles, prec_diag, low_factor, prior_mean, data_mat, labels):
        n_part, dim = particles.shape
        m_rows = data_mat.shape[0]
        rank = low_factor.shape[1]
        dim_full = dim * feat_size
        cfg = (chips, 2.0 * dim_full, dim_full / 4.0, 2.0 / math.sqrt(m_rows * dim_full))
        nb, mc = n_part // 2, m_rows // 2
        own = nb // feat_size
        vm, any_ = pl.BlockSpec(memory_space=pltpu.VMEM), pl.BlockSpec(memory_space=pl.ANY)
        dma = pltpu.SemaphoreType.DMA
        scratch = [
            pltpu.VMEM((n_part, dim), BF16), pltpu.VMEM((m_rows, dim), BF16),
            pltpu.VMEM((n_part, dim), F32), pltpu.VMEM((n_part, dim), BF16),
            pltpu.VMEM((n_part, n_part), BF16), pltpu.VMEM((n_part, LANES), F32), dma((4,)),
        ]
        for name in CHUNKS:
            wire, width, rows = (F32, LANES, own // 2 * 3) if name[0] == "g" else (BF16, mc, own)
            if name == "g1":
                rows = own // 2 * 7 + rank * n_part // LANES // feat_size
            count = len(DIRECT_KINDS if name in DIRECT else KINDS)
            scratch += [
                pltpu.VMEM((feat_size * rows, width), F32), pltpu.VMEM((chips * rows, width), F32),
                pltpu.VMEM((3 * rows, width), wire), pltpu.VMEM((3 * rows, width), wire),
                pltpu.VMEM((feat_size * rows, width), wire), dma((count,)), dma((count,)),
            ]
        return pl.pallas_call(
            functools.partial(kernel, cfg),
            out_shape=pltpu.VMEM((n_part, dim), F32),
            in_specs=[any_, vm, vm, vm, any_, vm],
            out_specs=vm,
            scratch_shapes=scratch,
            compiler_params=pltpu.CompilerParams(
                collective_id=0, has_side_effects=True, vmem_limit_bytes=48 * 2**20),
            cost_estimate=pl.CostEstimate(flops=60 * 10**9, bytes_accessed=32 * 2**20, transcendentals=0),
        )(particles, prec_diag[None, :], prior_mean[None, :], low_factor.T, data_mat, labels[None, :])

    return jax.shard_map(
        local_run,
        mesh=mesh,
        in_specs=(P("ens", "feat"), P(("ens", "feat")), P(("ens", "feat"), None),
                  P(("ens", "feat")), P("ens", "feat"), P("ens")),
        out_specs=P("ens", "feat"),
        check_vma=False,
    )
```

```python
import functools
import math
import jax
import jax.numpy as jnp
from jax import lax
from jax.experimental import pallas as pl
from jax.experimental.pallas import tpu as pltpu
from jax.sharding import PartitionSpec as P

NUM_STEPS = 3
CORES = 2
LANES = 128
F32, BF16 = jnp.float32, jnp.bfloat16
NN = (((1,), (0,)), ((), ()))
NT = (((1,), (1,)), ((), ()))
LOGICAL = pl.DeviceIdType.LOGICAL
KINDS = ("d2d", "s1a", "s1b", "ownb", "owna", "reda", "redb", "ir", "il", "io",
         "gr", "gl", "go", "gp", "fa", "flp", "fb", "frp", "fop")
CHUNKS = ("g0", "z0", "z3", "g1", "z1", "z2")
DIRECT = ('z0', 'z3', 'z1', 'z2', 'g0', 'g1')
GATHER_DIRECT = ('z1', 'z2', 'g0')
SCHEDULE = (
    "z0p", "z0:0", "gram0", "g0:0", "z0q", "z3:0", "z0:1", "drive1a", "drive1b", "g0:1", "gram1",
    "z3:1", "proj", "g1:0", "z0:3", "g1:1", "z1", "z1:0", "z3:3", "z0:4", "z2", "z1:1", "z2:0",
    "g1:3", "z3:4", "z2:1", "z1:3", "z0:5", "g1:4", "z3:5", "z0:6", "g0:3", "z3:6", "l0a", "z2:3",
    "z1:4", "z1:5", "l0b", "g1:5", "z1:6", "lf1a", "lf1b", "g0:4", "g0:5", "g1:6", "lr0", "lr1",
    "z2:4", "z2:5", "g0:6", "kmat", "d1", "d0", "z2:6", "ll1a", "ll1b", "drive0a", "drive0b",
)


def dot(a, b, dims=NN):
    return lax.dot_general(a, b, dims, preferred_element_type=F32)


class Chunk:
    def __init__(self, name, bufs, where, finish):
        self.part, self.pair, self.send, self.recv, self.full, self.ssem, self.rsem = bufs
        self.core, self.chip, self.chips, self.chip_of, self.ids = where
        self.rows = self.full.shape[0] // (CORES * self.chips)
        self.half = self.rows // 2 // 16 * 16
        self.direct = name in DIRECT
        self.gather_direct = name in GATHER_DIRECT
        unused = {"s1a", "s1b", "ownb", "owna", "reda", "redb"} if self.direct else {"ir", "il", "io"}
        unused |= {"fa", "fb"} if self.gather_direct else {"go"}
        self.kinds = [kind for kind in KINDS if kind not in unused]
        self.finish = finish

    def row(self, hop):
        return pl.multiple_of((self.core * self.chips + self.chip_of[hop]) * self.rows, 8)

    def copy(self, kind):
        rows, half = self.rows, self.half
        core, pair = self.core, self.ids["pair"]
        chip, right, left, opp = 0, 1, -1, 2
        at = lambda hop: self.ids[hop]
        snd, rcv, full = self.send, self.recv, self.full

        def same(lo, size):
            ref = full.at[pl.ds(lo, size), :]
            return ref, ref

        def slot(lo, hi):
            return snd.at[pl.ds(lo, hi - lo), :], rcv.at[pl.ds(lo, hi - lo), :]

        if kind == "d2d":
            size = self.chips * rows
            src, dst = self.part.at[pl.ds(pl.multiple_of((1 - core) * size, 8), size), :], self.pair
            dev = pair
        else:
            (src, dst), dev = {
                "s1a": lambda: (slot(0, half), at(right)),
                "s1b": lambda: (slot(half, rows), at(left)),
                "ownb": lambda: (slot(rows + half, 2 * rows), at(right)),
                "owna": lambda: (slot(2 * rows, 2 * rows + half), at(left)),
                "reda": lambda: (slot(rows, rows + half), at(right)),
                "redb": lambda: (slot(2 * rows + half, 3 * rows), at(left)),
                "io": lambda: (slot(0, rows), at(opp)),
                "ir": lambda: (slot(rows, 2 * rows), at(right)),
                "il": lambda: (slot(2 * rows, 3 * rows), at(left)),
                "gr": lambda: (same(self.row(chip), rows), at(right)),
                "gl": lambda: (same(self.row(chip), rows), at(left)),
                "go": lambda: (same(self.row(chip), rows), at(opp)),
                "gp": lambda: (same(self.row(chip), rows), pair),
                "fa": lambda: (same(self.row(left), half), at(right)),
                "flp": lambda: (same(self.row(left), rows), pair),
                "fb": lambda: (same(self.row(right) + half, rows - half), at(left)),
                "frp": lambda: (same(self.row(right), rows), pair),
                "fop": lambda: (same(self.row(opp), rows), pair),
            }[kind]()
        k = KINDS.index(kind)
        return pltpu.make_async_remote_copy(
            src_ref=src, dst_ref=dst, send_sem=self.ssem.at[k], recv_sem=self.rsem.at[k],
            device_id=dev, device_id_type=LOGICAL)

    def start(self, *kinds):
        for kind in kinds:
            self.copy(kind).start()

    def wait(self, *kinds):
        for kind in kinds:
            self.copy(kind).wait_recv()

    def mine(self, hop, lo, hi):
        a = self.part[pl.ds(self.row(hop) + lo, hi - lo), :]
        b = self.pair[pl.ds(pl.multiple_of(self.chip_of[hop] * self.rows, 8) + lo, hi - lo), :]
        return a + b

    def put(self, lo, value):
        self.send[lo:lo + value.shape[0], :] = value.astype(self.send.dtype)

    def got(self, lo, hi):
        return self.recv[lo:hi, :].astype(F32)

    def stage(self, n):
        rows, half = self.rows, self.half
        right, left, opp = 1, -1, 2
        if n == 0:
            self.start("d2d")
        elif n == 1:
            self.wait("d2d")
            self.put(0, self.mine(opp, 0, rows))
            if self.direct:
                self.start("io")
                self.put(rows, self.mine(right, 0, rows))
                self.start("ir")
                self.put(2 * rows, self.mine(left, 0, rows))
                self.start("il")
            else:
                self.start("s1a", "s1b")
                self.put(rows + half, self.mine(right, half, rows))
                self.start("ownb")
                self.put(2 * rows, self.mine(left, 0, half))
                self.start("owna")
        elif n == 2:
            self.wait("s1a")
            self.put(rows, self.mine(right, 0, half) + self.got(0, half))
            self.start("reda")
            self.wait("s1b")
            self.put(2 * rows + half, self.mine(left, half, rows) + self.got(half, rows))
            self.start("redb")
        elif n == 3:
            total = self.mine(0, 0, rows)
            if self.direct:
                self.wait("ir", "il", "io")
                total = total + self.got(rows, 2 * rows) + self.got(2 * rows, 3 * rows) + self.got(0, rows)
            else:
                self.wait("ownb", "owna", "reda", "redb")
                total = total + self.got(rows, 2 * rows) + self.got(2 * rows, 3 * rows)
            self.full[pl.ds(self.row(0), rows), :] = self.finish(total)
            if self.gather_direct:
                self.start("go")
            self.start("gr", "gl", "gp")
        elif n == 4:
            self.wait("gr")
            if not self.gather_direct:
                self.start("fa")
            self.start("flp")
            self.wait("gl")
            if not self.gather_direct:
                self.start("fb")
            self.start("frp")
        elif n == 5:
            if self.gather_direct:
                self.wait("go")
            else:
                self.wait("fa", "fb")
            self.start("fop")
        elif n == 6:
            self.wait("gp", "flp", "frp", "fop")

    def drain(self):
        for kind in self.kinds:
            self.copy(kind).wait_send()


def kernel(cfg, theta_hbm, lam_hbm, mu_hbm, ut_hbm, a_hbm, y_hbm, th, tb, av, sa, sb, kb, kv,
           lam_ref, mu_ref, ut_ref, y_ref, load_sem, small_sem, *chunk_bufs):
    chips, band, step, lik = cfg
    n_part, dim = th.shape
    m_rows = av.shape[0]
    nb, mc = n_part // 2, m_rows // 2
    owners = CORES * chips
    own = nb // owners
    wide, sub = dim // 2, 512
    blocks = [[(a, b) for a in (2 * i, 2 * i + 1) for b in range(a + 1)] for i in range(2)]
    share = LANES // owners
    q_row = len(blocks[1]) * share
    g1_piece = q_row + ut_ref.shape[0] // owners * (n_part // LANES)
    rank = ut_ref.shape[0]
    pull = 2.0 / band
    gain = step / n_part
    me = lax.axis_index("feat")
    core, chip = lax.rem(me, CORES), me // CORES
    group = lax.axis_index("ens") * owners
    chip_of = {hop: lax.rem(chip + hop + chips, chips) for hop in (-1, 0, 1, 2)}
    ids = {hop: group + chip_of[hop] * CORES + core for hop in (-1, 1, 2)}
    ids["pair"] = group + chip * CORES + (1 - core)
    where = (core, chip, chips, chip_of, ids)

    def finish(name):
        if name[0] == "g":
            return lambda g: g
        lo = 0 if name in ("z0", "z1") else mc

        def residual(z):
            return (y_ref[:, lo:lo + mc].astype(F32) - 1.0 / (1.0 + jnp.exp(-z))).astype(BF16)
        return residual

    ch = {}
    for k, name in enumerate(CHUNKS):
        ch[name] = Chunk(name, chunk_bufs[7 * k:7 * k + 7], where, finish(name))

    def rows(i):
        return slice(i * nb, (i + 1) * nb)

    def load_theta(i):
        return pltpu.make_async_copy(theta_hbm.at[pl.ds(i * nb, nb), :], th.at[pl.ds(i * nb, nb), :], load_sem.at[i])

    def load_a(j):
        return pltpu.make_async_copy(a_hbm.at[pl.ds(j * mc, mc), :], av.at[pl.ds(j * mc, mc), :], load_sem.at[2 + j])

    load_theta(0).start()
    load_a(0).start()
    load_a(1).start()
    load_theta(1).start()
    small = [pltpu.make_async_copy(src, dst, small_sem.at[k]) for k, (src, dst) in enumerate(
        ((lam_hbm, lam_ref), (mu_hbm, mu_ref), (ut_hbm, ut_ref), (y_hbm, y_ref)))]
    for copy in small:
        copy.start()

    barrier = pltpu.get_barrier_semaphore()
    for peer in ids.values():
        pl.semaphore_signal(barrier, inc=1, device_id=peer, device_id_type=LOGICAL)
    pl.semaphore_wait(barrier, len(ids))

    def columns(lo, hi):
        return [slice(n, n + sub) for n in range(lo, hi, sub)]

    def prep(i):
        load_theta(i).wait()

        @pl.loop(0, dim // wide)
        def _(t):
            n = pl.ds(pl.multiple_of(t * wide, wide), wide)
            tb[rows(i), n] = th[rows(i), n].astype(BF16)

    def project():
        q = jnp.zeros((rank, n_part), F32)
        for n in columns(0, dim):
            q = q + dot(ut_ref[:, n], (th[:, n] - mu_ref[:, n]).astype(BF16), NT)
        part = rank // owners
        for o in range(owners):
            for k in range(n_part // LANES):
                lo = o * g1_piece + q_row + k * part
                ch["g1"].part[lo:lo + part, :] = q[o * part:(o + 1) * part, k * LANES:(k + 1) * LANES]

    def gram(i):
        g = dot(tb[rows(i), :], tb[0:(i + 1) * nb, :], NT)
        part = ch[f"g{i}"].part
        piece = part.shape[0] // owners
        for k, (a, b) in enumerate(blocks[i]):
            block = g[(a - 2 * i) * LANES:(a - 2 * i + 1) * LANES, b * LANES:(b + 1) * LANES]
            for o in range(owners):
                part[o * piece + k * share:o * piece + (k + 1) * share, :] = block[o * share:(o + 1) * share]

    def logit(name, i, j):
        ch[name].part[...] = dot(tb[rows(i), :], av[j * mc:(j + 1) * mc, :], NT)

    def base(i, n, q):
        x = th[rows(i), n] - mu_ref[:, n]
        return x * lam_ref[:, n] + dot(q, ut_ref[:, n]) + pull * tb[rows(i), n].astype(F32)

    def gathered_q(i):
        part = rank // owners
        parts = []
        for k in range(i * nb // LANES, (i + 1) * nb // LANES):
            los = [o * g1_piece + q_row + k * part for o in range(owners)]
            parts.append(jnp.concatenate([ch["g1"].full[lo:lo + part, :] for lo in los], axis=0).T)
        return jnp.concatenate(parts, axis=0).astype(BF16)

    def both_lik(lo, hi):
        for n in columns(lo, hi):
            sa[rows(0), n] = lik * (dot(ch["z0"].full[...], av[0:mc, n]) + dot(ch["z3"].full[...], av[mc:2 * mc, n]))

    def first_lik(lo, hi):
        for n in columns(lo, hi):
            sa[rows(1), n] = lik * dot(ch["z1"].full[...], av[0:mc, n])

    def last_lik(lo, hi):
        for n in columns(lo, hi):
            sb[rows(1), n] = (sa[rows(1), n] + lik * dot(ch["z2"].full[...], av[mc:2 * mc, n])).astype(BF16)

    def low_rank(i):
        q = gathered_q(i)
        for n in columns(0, dim):
            s = sa[rows(i), n] - base(i, n, q)
            if i == 0:
                sb[rows(i), n] = s.astype(BF16)
            else:
                sa[rows(i), n] = s

    def kernel_mat():
        grams = {}
        for i in range(2):
            full = ch[f"g{i}"].full
            piece = full.shape[0] // owners
            for k, ab in enumerate(blocks[i]):
                grams[ab] = jnp.concatenate(
                    [full[o * piece + k * share:o * piece + (k + 1) * share, :] for o in range(owners)], axis=0)
        eye = lax.broadcasted_iota(jnp.int32, (LANES, LANES), 0) == lax.broadcasted_iota(jnp.int32, (LANES, LANES), 1)
        count = n_part // LANES
        norms = [jnp.where(eye, grams[a, a], 0.0) for a in range(count)]
        cols = [jnp.sum(d, axis=1, keepdims=True) for d in norms]
        lines = [jnp.sum(d, axis=0, keepdims=True) for d in norms]
        totals = [0.0] * count
        for (a, b), g in grams.items():
            k = jnp.exp(-jnp.maximum(cols[a] + lines[b] - 2.0 * g, 0.0) / band)
            for i, j, m in ((a, b, k), (b, a, k.T))[:2 if a != b else 1]:
                kb[i * LANES:(i + 1) * LANES, j * LANES:(j + 1) * LANES] = m.astype(BF16)
                totals[i] = totals[i] + jnp.sum(m, axis=1, keepdims=True)
        for a in range(count):
            kv[a * LANES:(a + 1) * LANES, :] = jnp.broadcast_to(gain * pull * totals[a], (LANES, LANES))

    def drive_first(i):
        for n in columns(0, dim):
            t = th[rows(i), n]
            scale = jnp.concatenate([kv[rows(i), :]] * (sub // LANES), axis=1)
            th[rows(i), n] = t + (scale * t + gain * dot(kb[rows(i), rows(0)], sb[rows(0), n]))

    def drive(i, lo, hi):
        for n in columns(lo, hi):
            t = th[rows(i), n] + gain * dot(kb[rows(i), rows(1)], sb[rows(1), n])
            th[rows(i), n] = t
            tb[rows(i), n] = t.astype(BF16)

    halves = {"a": (0, wide), "b": (wide, dim)}
    pieces = {
        "proj": project, "gram0": lambda: gram(0), "gram1": lambda: gram(1),
        "z0p": lambda: logit("z0", 0, 0), "z0q": lambda: logit("z3", 0, 1),
        "z1": lambda: logit("z1", 1, 0), "z2": lambda: logit("z2", 1, 1),
        "lr0": lambda: low_rank(0), "lr1": lambda: low_rank(1), "kmat": kernel_mat,
        "d0": lambda: drive_first(0), "d1": lambda: drive_first(1),
    }
    for h, (lo, hi) in halves.items():
        pieces["l0" + h] = functools.partial(both_lik, lo, hi)
        pieces["lf1" + h] = functools.partial(first_lik, lo, hi)
        pieces["ll1" + h] = functools.partial(last_lik, lo, hi)
        pieces["drive0" + h] = functools.partial(drive, 0, lo, hi)
        pieces["drive1" + h] = functools.partial(drive, 1, lo, hi)

    @pl.loop(0, NUM_STEPS)
    def _(s):
        @pl.when(s == 0)
        def _():
            for copy in small:
                copy.wait()
            prep(0)

        loaded = set()
        for item in SCHEDULE:
            if ":" in item:
                name, n = item.split(":")
                ch[name].stage(int(n))
                continue
            if item in ("z0p", "z0q"):
                @pl.when(s == 0)
                def _():
                    load_a("pq".index(item[-1])).wait()
            if item == "drive1a":
                @pl.when(s == 0)
                def _():
                    prep(1)
            if item[:6] == "drive1":
                pl.when(s > 0)(pieces[item])
            else:
                pieces[item]()
        for name in CHUNKS:
            ch[name].drain()

    for lo, hi in halves.values():
        drive(1, lo, hi)


def solution(mesh):
    feat_size = mesh.shape["feat"]
    chips = feat_size // CORES

    def local_run(particles, prec_diag, low_factor, prior_mean, data_mat, labels):
        n_part, dim = particles.shape
        m_rows = data_mat.shape[0]
        rank = low_factor.shape[1]
        dim_full = dim * feat_size
        cfg = (chips, 2.0 * dim_full, dim_full / 4.0, 2.0 / math.sqrt(m_rows * dim_full))
        nb, mc = n_part // 2, m_rows // 2
        own = nb // feat_size
        vm, any_ = pl.BlockSpec(memory_space=pltpu.VMEM), pl.BlockSpec(memory_space=pl.ANY)
        dma = pltpu.SemaphoreType.DMA
        scratch = [
            pltpu.VMEM((n_part, dim), BF16), pltpu.VMEM((m_rows, dim), BF16),
            pltpu.VMEM((n_part, dim), F32), pltpu.VMEM((n_part, dim), BF16),
            pltpu.VMEM((n_part, n_part), BF16), pltpu.VMEM((n_part, LANES), F32),
            pltpu.VMEM((1, dim), F32), pltpu.VMEM((1, dim), F32), pltpu.VMEM((rank, dim), BF16),
            pltpu.VMEM((1, m_rows), jnp.int32), dma((4,)), dma((4,)),
        ]
        for name in CHUNKS:
            wire, width, rows = (F32, LANES, own // 2 * 3) if name[0] == "g" else (BF16, mc, own)
            if name == "g1":
                rows = own // 2 * 7 + rank * n_part // LANES // feat_size
            scratch += [
                pltpu.VMEM((feat_size * rows, width), F32), pltpu.VMEM((chips * rows, width), F32),
                pltpu.VMEM((3 * rows, width), wire), pltpu.VMEM((3 * rows, width), wire),
                pltpu.VMEM((feat_size * rows, width), wire), dma((len(KINDS),)), dma((len(KINDS),)),
            ]
        return pl.pallas_call(
            functools.partial(kernel, cfg),
            out_shape=pltpu.VMEM((n_part, dim), F32),
            in_specs=[any_] * 6,
            out_specs=vm,
            scratch_shapes=scratch,
            compiler_params=pltpu.CompilerParams(
                collective_id=0, has_side_effects=True, vmem_limit_bytes=48 * 2**20),
            cost_estimate=pl.CostEstimate(flops=60 * 10**9, bytes_accessed=32 * 2**20, transcendentals=0),
        )(particles, prec_diag[None, :], prior_mean[None, :], low_factor.T, data_mat, labels[None, :])

    return jax.shard_map(
        local_run,
        mesh=mesh,
        in_specs=(P("ens", "feat"), P(("ens", "feat")), P(("ens", "feat"), None),
                  P(("ens", "feat")), P("ens", "feat"), P("ens")),
        out_specs=P("ens", "feat"),
        check_vma=False,
    )
```

```python
import functools
import math
import jax
import jax.numpy as jnp
from jax import lax
from jax.experimental import pallas as pl
from jax.experimental.pallas import tpu as pltpu
from jax.sharding import PartitionSpec as P

NUM_STEPS = 3
CORES = 2
LANES = 128
F32, BF16 = jnp.float32, jnp.bfloat16
NN = (((1,), (0,)), ((), ()))
NT = (((1,), (1,)), ((), ()))
LOGICAL = pl.DeviceIdType.LOGICAL
KINDS = ("d2d", "s1a", "s1b", "ownb", "owna", "reda", "redb", "ir", "il", "io",
         "gr", "gl", "go", "gp", "fa", "flp", "fb", "frp", "fop")
CHUNKS = ("g0", "z0", "z3", "g1", "z1", "z2")
DIRECT = ('z0', 'z3', 'z1', 'z2', 'g0', 'g1')
GATHER_DIRECT = ('z0', 'z3', 'z1', 'z2', 'g0', 'g1')
SCHEDULE = (
    "z0p", "z0:0", "drive1a", "z0q", "z3:0", "z0:1", "drive1b", "gram0", "g0:0", "z1", "z1:0", "z3:1",
    "gram1", "g0:1", "z1:1", "proj", "g1:0", "z0:3", "g1:1", "z2", "z2:0", "z3:3", "z2:1", "g0:3",
    "z1:3", "g1:3", "z0:4", "z0:5", "z3:4", "z3:5", "z3:6", "z0:6", "z2:3", "l0a", "g0:4", "g0:5",
    "z1:4", "z1:5", "l0b", "z1:6", "lf1a", "g0:6", "g1:4", "g1:5", "lf1b", "z2:4", "z2:5", "g1:6",
    "kmat", "lr0", "z2:6", "lr1", "d1", "d0", "ll1a", "ll1b", "drive0a", "drive0b",
)


def dot(a, b, dims=NN):
    return lax.dot_general(a, b, dims, preferred_element_type=F32)


class Chunk:
    def __init__(self, name, bufs, where, finish):
        self.part, self.pair, self.send, self.recv, self.full, self.ssem, self.rsem = bufs
        self.core, self.chip, self.chips, self.chip_of, self.ids = where
        self.rows = self.full.shape[0] // (CORES * self.chips)
        self.half = self.rows // 2 // 16 * 16
        self.direct = name in DIRECT
        self.gather_direct = name in GATHER_DIRECT
        unused = {"s1a", "s1b", "ownb", "owna", "reda", "redb"} if self.direct else {"ir", "il", "io"}
        unused |= {"fa", "fb"} if self.gather_direct else {"go"}
        self.kinds = [kind for kind in KINDS if kind not in unused]
        self.finish = finish

    def row(self, hop):
        return pl.multiple_of((self.core * self.chips + self.chip_of[hop]) * self.rows, 8)

    def copy(self, kind):
        rows, half = self.rows, self.half
        core, pair = self.core, self.ids["pair"]
        chip, right, left, opp = 0, 1, -1, 2
        at = lambda hop: self.ids[hop]
        snd, rcv, full = self.send, self.recv, self.full

        def same(lo, size):
            ref = full.at[pl.ds(lo, size), :]
            return ref, ref

        def slot(lo, hi):
            return snd.at[pl.ds(lo, hi - lo), :], rcv.at[pl.ds(lo, hi - lo), :]

        if kind == "d2d":
            size = self.chips * rows
            src, dst = self.part.at[pl.ds(pl.multiple_of((1 - core) * size, 8), size), :], self.pair
            dev = pair
        else:
            (src, dst), dev = {
                "s1a": lambda: (slot(0, half), at(right)),
                "s1b": lambda: (slot(half, rows), at(left)),
                "ownb": lambda: (slot(rows + half, 2 * rows), at(right)),
                "owna": lambda: (slot(2 * rows, 2 * rows + half), at(left)),
                "reda": lambda: (slot(rows, rows + half), at(right)),
                "redb": lambda: (slot(2 * rows + half, 3 * rows), at(left)),
                "io": lambda: (slot(0, rows), at(opp)),
                "ir": lambda: (slot(rows, 2 * rows), at(right)),
                "il": lambda: (slot(2 * rows, 3 * rows), at(left)),
                "gr": lambda: (same(self.row(chip), rows), at(right)),
                "gl": lambda: (same(self.row(chip), rows), at(left)),
                "go": lambda: (same(self.row(chip), rows), at(opp)),
                "gp": lambda: (same(self.row(chip), rows), pair),
                "fa": lambda: (same(self.row(left), half), at(right)),
                "flp": lambda: (same(self.row(left), rows), pair),
                "fb": lambda: (same(self.row(right) + half, rows - half), at(left)),
                "frp": lambda: (same(self.row(right), rows), pair),
                "fop": lambda: (same(self.row(opp), rows), pair),
            }[kind]()
        k = KINDS.index(kind)
        return pltpu.make_async_remote_copy(
            src_ref=src, dst_ref=dst, send_sem=self.ssem.at[k], recv_sem=self.rsem.at[k],
            device_id=dev, device_id_type=LOGICAL)

    def start(self, *kinds):
        for kind in kinds:
            self.copy(kind).start()

    def wait(self, *kinds):
        for kind in kinds:
            self.copy(kind).wait_recv()

    def mine(self, hop, lo, hi):
        a = self.part[pl.ds(self.row(hop) + lo, hi - lo), :]
        b = self.pair[pl.ds(pl.multiple_of(self.chip_of[hop] * self.rows, 8) + lo, hi - lo), :]
        return a + b

    def put(self, lo, value):
        self.send[lo:lo + value.shape[0], :] = value.astype(self.send.dtype)

    def got(self, lo, hi):
        return self.recv[lo:hi, :].astype(F32)

    def stage(self, n):
        rows, half = self.rows, self.half
        right, left, opp = 1, -1, 2
        if n == 0:
            self.start("d2d")
        elif n == 1:
            self.wait("d2d")
            self.put(0, self.mine(opp, 0, rows))
            if self.direct:
                self.start("io")
                self.put(rows, self.mine(right, 0, rows))
                self.start("ir")
                self.put(2 * rows, self.mine(left, 0, rows))
                self.start("il")
            else:
                self.start("s1a", "s1b")
                self.put(rows + half, self.mine(right, half, rows))
                self.start("ownb")
                self.put(2 * rows, self.mine(left, 0, half))
                self.start("owna")
        elif n == 2:
            self.wait("s1a")
            self.put(rows, self.mine(right, 0, half) + self.got(0, half))
            self.start("reda")
            self.wait("s1b")
            self.put(2 * rows + half, self.mine(left, half, rows) + self.got(half, rows))
            self.start("redb")
        elif n == 3:
            total = self.mine(0, 0, rows)
            if self.direct:
                self.wait("ir", "il", "io")
                total = total + self.got(rows, 2 * rows) + self.got(2 * rows, 3 * rows) + self.got(0, rows)
            else:
                self.wait("ownb", "owna", "reda", "redb")
                total = total + self.got(rows, 2 * rows) + self.got(2 * rows, 3 * rows)
            self.full[pl.ds(self.row(0), rows), :] = self.finish(total)
            if self.gather_direct:
                self.start("go")
            self.start("gr", "gl", "gp")
        elif n == 4:
            self.wait("gr")
            if not self.gather_direct:
                self.start("fa")
            self.start("flp")
            self.wait("gl")
            if not self.gather_direct:
                self.start("fb")
            self.start("frp")
        elif n == 5:
            if self.gather_direct:
                self.wait("go")
            else:
                self.wait("fa", "fb")
            self.start("fop")
        elif n == 6:
            self.wait("gp", "flp", "frp", "fop")

    def drain(self):
        for kind in self.kinds:
            self.copy(kind).wait_send()


def kernel(cfg, theta_hbm, lam_hbm, mu_hbm, ut_hbm, a_hbm, y_hbm, th, tb, av, sa, sb, kb, kv,
           lam_ref, mu_ref, ut_ref, y_ref, load_sem, small_sem, *chunk_bufs):
    chips, band, step, lik = cfg
    n_part, dim = th.shape
    m_rows = av.shape[0]
    nb, mc = n_part // 2, m_rows // 2
    owners = CORES * chips
    own = nb // owners
    wide, sub = dim // 2, 512
    blocks = [[(a, b) for a in (2 * i, 2 * i + 1) for b in range(a + 1)] for i in range(2)]
    share = LANES // owners
    q_row = len(blocks[1]) * share
    g1_piece = q_row + ut_ref.shape[0] // owners * (n_part // LANES)
    rank = ut_ref.shape[0]
    pull = 2.0 / band
    gain = step / n_part
    me = lax.axis_index("feat")
    core, chip = lax.rem(me, CORES), me // CORES
    group = lax.axis_index("ens") * owners
    chip_of = {hop: lax.rem(chip + hop + chips, chips) for hop in (-1, 0, 1, 2)}
    ids = {hop: group + chip_of[hop] * CORES + core for hop in (-1, 1, 2)}
    ids["pair"] = group + chip * CORES + (1 - core)
    where = (core, chip, chips, chip_of, ids)

    def finish(name):
        if name[0] == "g":
            return lambda g: g
        lo = 0 if name in ("z0", "z1") else mc

        def residual(z):
            return (y_ref[:, lo:lo + mc].astype(F32) - 1.0 / (1.0 + jnp.exp(-z))).astype(BF16)
        return residual

    ch = {}
    for k, name in enumerate(CHUNKS):
        ch[name] = Chunk(name, chunk_bufs[7 * k:7 * k + 7], where, finish(name))

    def rows(i):
        return slice(i * nb, (i + 1) * nb)

    def load_theta(i):
        return pltpu.make_async_copy(theta_hbm.at[pl.ds(i * nb, nb), :], th.at[pl.ds(i * nb, nb), :], load_sem.at[i])

    def load_a(j):
        return pltpu.make_async_copy(a_hbm.at[pl.ds(j * mc, mc), :], av.at[pl.ds(j * mc, mc), :], load_sem.at[2 + j])

    load_theta(0).start()
    load_a(0).start()
    load_a(1).start()
    load_theta(1).start()
    small = [pltpu.make_async_copy(src, dst, small_sem.at[k]) for k, (src, dst) in enumerate(
        ((lam_hbm, lam_ref), (mu_hbm, mu_ref), (ut_hbm, ut_ref), (y_hbm, y_ref)))]
    for copy in small:
        copy.start()

    barrier = pltpu.get_barrier_semaphore()
    for peer in ids.values():
        pl.semaphore_signal(barrier, inc=1, device_id=peer, device_id_type=LOGICAL)
    pl.semaphore_wait(barrier, len(ids))

    def columns(lo, hi):
        return [slice(n, n + sub) for n in range(lo, hi, sub)]

    def prep(i):
        load_theta(i).wait()

        @pl.loop(0, dim // wide)
        def _(t):
            n = pl.ds(pl.multiple_of(t * wide, wide), wide)
            tb[rows(i), n] = th[rows(i), n].astype(BF16)

    def project():
        q = jnp.zeros((rank, n_part), F32)
        for n in columns(0, dim):
            q = q + dot(ut_ref[:, n], (th[:, n] - mu_ref[:, n]).astype(BF16), NT)
        part = rank // owners
        for o in range(owners):
            for k in range(n_part // LANES):
                lo = o * g1_piece + q_row + k * part
                ch["g1"].part[lo:lo + part, :] = q[o * part:(o + 1) * part, k * LANES:(k + 1) * LANES]

    def gram(i):
        g = dot(tb[rows(i), :], tb[0:(i + 1) * nb, :], NT)
        part = ch[f"g{i}"].part
        piece = part.shape[0] // owners
        for k, (a, b) in enumerate(blocks[i]):
            block = g[(a - 2 * i) * LANES:(a - 2 * i + 1) * LANES, b * LANES:(b + 1) * LANES]
            for o in range(owners):
                part[o * piece + k * share:o * piece + (k + 1) * share, :] = block[o * share:(o + 1) * share]

    def logit(name, i, j):
        ch[name].part[...] = dot(tb[rows(i), :], av[j * mc:(j + 1) * mc, :], NT)

    def base(i, n, q):
        x = th[rows(i), n] - mu_ref[:, n]
        return x * lam_ref[:, n] + dot(q, ut_ref[:, n]) + pull * tb[rows(i), n].astype(F32)

    def gathered_q(i):
        part = rank // owners
        parts = []
        for k in range(i * nb // LANES, (i + 1) * nb // LANES):
            los = [o * g1_piece + q_row + k * part for o in range(owners)]
            parts.append(jnp.concatenate([ch["g1"].full[lo:lo + part, :] for lo in los], axis=0).T)
        return jnp.concatenate(parts, axis=0).astype(BF16)

    def both_lik(lo, hi):
        for n in columns(lo, hi):
            sa[rows(0), n] = lik * (dot(ch["z0"].full[...], av[0:mc, n]) + dot(ch["z3"].full[...], av[mc:2 * mc, n]))

    def first_lik(lo, hi):
        for n in columns(lo, hi):
            sa[rows(1), n] = lik * dot(ch["z1"].full[...], av[0:mc, n])

    def last_lik(lo, hi):
        for n in columns(lo, hi):
            sb[rows(1), n] = (sa[rows(1), n] + lik * dot(ch["z2"].full[...], av[mc:2 * mc, n])).astype(BF16)

    def low_rank(i):
        q = gathered_q(i)
        for n in columns(0, dim):
            s = sa[rows(i), n] - base(i, n, q)
            if i == 0:
                sb[rows(i), n] = s.astype(BF16)
            else:
                sa[rows(i), n] = s

    def kernel_mat():
        grams = {}
        for i in range(2):
            full = ch[f"g{i}"].full
            piece = full.shape[0] // owners
            for k, ab in enumerate(blocks[i]):
                grams[ab] = jnp.concatenate(
                    [full[o * piece + k * share:o * piece + (k + 1) * share, :] for o in range(owners)], axis=0)
        eye = lax.broadcasted_iota(jnp.int32, (LANES, LANES), 0) == lax.broadcasted_iota(jnp.int32, (LANES, LANES), 1)
        count = n_part // LANES
        norms = [jnp.where(eye, grams[a, a], 0.0) for a in range(count)]
        cols = [jnp.sum(d, axis=1, keepdims=True) for d in norms]
        lines = [jnp.sum(d, axis=0, keepdims=True) for d in norms]
        totals = [0.0] * count
        for (a, b), g in grams.items():
            k = jnp.exp(-jnp.maximum(cols[a] + lines[b] - 2.0 * g, 0.0) / band)
            for i, j, m in ((a, b, k), (b, a, k.T))[:2 if a != b else 1]:
                kb[i * LANES:(i + 1) * LANES, j * LANES:(j + 1) * LANES] = m.astype(BF16)
                totals[i] = totals[i] + jnp.sum(m, axis=1, keepdims=True)
        for a in range(count):
            kv[a * LANES:(a + 1) * LANES, :] = jnp.broadcast_to(gain * pull * totals[a], (LANES, LANES))

    def drive_first(i):
        for n in columns(0, dim):
            t = th[rows(i), n]
            scale = jnp.concatenate([kv[rows(i), :]] * (sub // LANES), axis=1)
            th[rows(i), n] = t + (scale * t + gain * dot(kb[rows(i), rows(0)], sb[rows(0), n]))

    def drive(i, lo, hi):
        for n in columns(lo, hi):
            t = th[rows(i), n] + gain * dot(kb[rows(i), rows(1)], sb[rows(1), n])
            th[rows(i), n] = t
            tb[rows(i), n] = t.astype(BF16)

    halves = {"a": (0, wide), "b": (wide, dim)}
    pieces = {
        "proj": project, "gram0": lambda: gram(0), "gram1": lambda: gram(1),
        "z0p": lambda: logit("z0", 0, 0), "z0q": lambda: logit("z3", 0, 1),
        "z1": lambda: logit("z1", 1, 0), "z2": lambda: logit("z2", 1, 1),
        "lr0": lambda: low_rank(0), "lr1": lambda: low_rank(1), "kmat": kernel_mat,
        "d0": lambda: drive_first(0), "d1": lambda: drive_first(1),
    }
    for h, (lo, hi) in halves.items():
        pieces["l0" + h] = functools.partial(both_lik, lo, hi)
        pieces["lf1" + h] = functools.partial(first_lik, lo, hi)
        pieces["ll1" + h] = functools.partial(last_lik, lo, hi)
        pieces["drive0" + h] = functools.partial(drive, 0, lo, hi)
        pieces["drive1" + h] = functools.partial(drive, 1, lo, hi)

    @pl.loop(0, NUM_STEPS)
    def _(s):
        @pl.when(s == 0)
        def _():
            for copy in small:
                copy.wait()
            prep(0)

        loaded = set()
        for item in SCHEDULE:
            if ":" in item:
                name, n = item.split(":")
                ch[name].stage(int(n))
                continue
            if item in ("z0p", "z0q"):
                @pl.when(s == 0)
                def _():
                    load_a("pq".index(item[-1])).wait()
            if item == "drive1a":
                @pl.when(s == 0)
                def _():
                    prep(1)
            if item[:6] == "drive1":
                pl.when(s > 0)(pieces[item])
            else:
                pieces[item]()
        for name in CHUNKS:
            ch[name].drain()

    for lo, hi in halves.values():
        drive(1, lo, hi)


def solution(mesh):
    feat_size = mesh.shape["feat"]
    chips = feat_size // CORES

    def local_run(particles, prec_diag, low_factor, prior_mean, data_mat, labels):
        n_part, dim = particles.shape
        m_rows = data_mat.shape[0]
        rank = low_factor.shape[1]
        dim_full = dim * feat_size
        cfg = (chips, 2.0 * dim_full, dim_full / 4.0, 2.0 / math.sqrt(m_rows * dim_full))
        nb, mc = n_part // 2, m_rows // 2
        own = nb // feat_size
        vm, any_ = pl.BlockSpec(memory_space=pltpu.VMEM), pl.BlockSpec(memory_space=pl.ANY)
        dma = pltpu.SemaphoreType.DMA
        scratch = [
            pltpu.VMEM((n_part, dim), BF16), pltpu.VMEM((m_rows, dim), BF16),
            pltpu.VMEM((n_part, dim), F32), pltpu.VMEM((n_part, dim), BF16),
            pltpu.VMEM((n_part, n_part), BF16), pltpu.VMEM((n_part, LANES), F32),
            pltpu.VMEM((1, dim), F32), pltpu.VMEM((1, dim), F32), pltpu.VMEM((rank, dim), BF16),
            pltpu.VMEM((1, m_rows), jnp.int32), dma((4,)), dma((4,)),
        ]
        for name in CHUNKS:
            wire, width, rows = (F32, LANES, own // 2 * 3) if name[0] == "g" else (BF16, mc, own)
            if name == "g1":
                rows = own // 2 * 7 + rank * n_part // LANES // feat_size
            scratch += [
                pltpu.VMEM((feat_size * rows, width), F32), pltpu.VMEM((chips * rows, width), F32),
                pltpu.VMEM((3 * rows, width), wire), pltpu.VMEM((3 * rows, width), wire),
                pltpu.VMEM((feat_size * rows, width), wire), dma((len(KINDS),)), dma((len(KINDS),)),
            ]
        return pl.pallas_call(
            functools.partial(kernel, cfg),
            out_shape=pltpu.VMEM((n_part, dim), F32),
            in_specs=[any_] * 6,
            out_specs=vm,
            scratch_shapes=scratch,
            compiler_params=pltpu.CompilerParams(
                collective_id=0, has_side_effects=True, vmem_limit_bytes=48 * 2**20),
            cost_estimate=pl.CostEstimate(flops=60 * 10**9, bytes_accessed=32 * 2**20, transcendentals=0),
        )(particles, prec_diag[None, :], prior_mean[None, :], low_factor.T, data_mat, labels[None, :])

    return jax.shard_map(
        local_run,
        mesh=mesh,
        in_specs=(P("ens", "feat"), P(("ens", "feat")), P(("ens", "feat"), None),
                  P(("ens", "feat")), P("ens", "feat"), P("ens")),
        out_specs=P("ens", "feat"),
        check_vma=False,
    )
```

```python
import functools
import math
import jax
import jax.numpy as jnp
from jax import lax
from jax.experimental import pallas as pl
from jax.experimental.pallas import tpu as pltpu
from jax.sharding import PartitionSpec as P

NUM_STEPS = 3
CORES = 2
LANES = 128
F32, BF16 = jnp.float32, jnp.bfloat16
NN = (((1,), (0,)), ((), ()))
NT = (((1,), (1,)), ((), ()))
LOGICAL = pl.DeviceIdType.LOGICAL
KINDS = ("d2d", "s1a", "s1b", "ownb", "owna", "reda", "redb", "ir", "il", "io",
         "gr", "gl", "go", "gp", "fa", "flp", "fb", "frp", "fop")
CHUNKS = ("g0", "z0", "z3", "g1", "z1", "z2")
DIRECT = ('z0', 'z3', 'z1', 'z2', 'g0', 'g1')
GATHER_DIRECT = ('z0', 'z3', 'z1', 'z2', 'g0', 'g1')
SCHEDULE = (
    "z0p", "z0:0", "drive1a", "z0q", "z3:0", "z0:1", "drive1b", "gram0", "g0:0", "z1", "z1:0", "z3:1",
    "gram1", "g0:1", "z1:1", "proj", "g1:0", "z0:3", "g1:1", "z2", "z2:0", "z3:3", "z2:1", "g0:3",
    "z1:3", "g1:3", "z0:4", "z0:5", "z3:4", "z3:5", "z3:6", "z0:6", "z2:3", "l0a", "g0:4", "g0:5",
    "z1:4", "z1:5", "l0b", "z1:6", "lf1a", "g0:6", "g1:4", "g1:5", "lf1b", "z2:4", "z2:5", "g1:6",
    "kmat", "lr0", "z2:6", "lr1", "d1", "d0", "ll1a", "ll1b", "drive0a", "drive0b",
)


def dot(a, b, dims=NN):
    return lax.dot_general(a, b, dims, preferred_element_type=F32)


class Chunk:
    def __init__(self, name, bufs, where, finish):
        self.part, self.pair, self.send, self.recv, self.full, self.ssem, self.rsem = bufs
        self.core, self.chip, self.chips, self.chip_of, self.ids = where
        self.rows = self.full.shape[0] // (CORES * self.chips)
        self.half = self.rows // 2 // 16 * 16
        self.direct = name in DIRECT
        self.gather_direct = name in GATHER_DIRECT
        unused = {"s1a", "s1b", "ownb", "owna", "reda", "redb"} if self.direct else {"ir", "il", "io"}
        unused |= {"fa", "fb"} if self.gather_direct else {"go"}
        self.kinds = [kind for kind in KINDS if kind not in unused]
        self.finish = finish

    def row(self, hop):
        return pl.multiple_of((self.core * self.chips + self.chip_of[hop]) * self.rows, 8)

    def copy(self, kind):
        rows, half = self.rows, self.half
        core, pair = self.core, self.ids["pair"]
        chip, right, left, opp = 0, 1, -1, 2
        at = lambda hop: self.ids[hop]
        snd, rcv, full = self.send, self.recv, self.full

        def same(lo, size):
            ref = full.at[pl.ds(lo, size), :]
            return ref, ref

        def slot(lo, hi):
            return snd.at[pl.ds(lo, hi - lo), :], rcv.at[pl.ds(lo, hi - lo), :]

        if kind == "d2d":
            size = self.chips * rows
            src, dst = self.part.at[pl.ds(pl.multiple_of((1 - core) * size, 8), size), :], self.pair
            dev = pair
        else:
            (src, dst), dev = {
                "s1a": lambda: (slot(0, half), at(right)),
                "s1b": lambda: (slot(half, rows), at(left)),
                "ownb": lambda: (slot(rows + half, 2 * rows), at(right)),
                "owna": lambda: (slot(2 * rows, 2 * rows + half), at(left)),
                "reda": lambda: (slot(rows, rows + half), at(right)),
                "redb": lambda: (slot(2 * rows + half, 3 * rows), at(left)),
                "io": lambda: (slot(0, rows), at(opp)),
                "ir": lambda: (slot(rows, 2 * rows), at(right)),
                "il": lambda: (slot(2 * rows, 3 * rows), at(left)),
                "gr": lambda: (same(self.row(chip), rows), at(right)),
                "gl": lambda: (same(self.row(chip), rows), at(left)),
                "go": lambda: (same(self.row(chip), rows), at(opp)),
                "gp": lambda: (same(self.row(chip), rows), pair),
                "fa": lambda: (same(self.row(left), half), at(right)),
                "flp": lambda: (same(self.row(left), rows), pair),
                "fb": lambda: (same(self.row(right) + half, rows - half), at(left)),
                "frp": lambda: (same(self.row(right), rows), pair),
                "fop": lambda: (same(self.row(opp), rows), pair),
            }[kind]()
        k = KINDS.index(kind)
        return pltpu.make_async_remote_copy(
            src_ref=src, dst_ref=dst, send_sem=self.ssem.at[k], recv_sem=self.rsem.at[k],
            device_id=dev, device_id_type=LOGICAL)

    def start(self, *kinds):
        for kind in kinds:
            self.copy(kind).start()

    def wait(self, *kinds):
        for kind in kinds:
            self.copy(kind).wait_recv()

    def mine(self, hop, lo, hi):
        a = self.part[pl.ds(self.row(hop) + lo, hi - lo), :]
        b = self.pair[pl.ds(pl.multiple_of(self.chip_of[hop] * self.rows, 8) + lo, hi - lo), :]
        return a + b

    def put(self, lo, value):
        self.send[lo:lo + value.shape[0], :] = value.astype(self.send.dtype)

    def got(self, lo, hi):
        return self.recv[lo:hi, :].astype(F32)

    def stage(self, n):
        rows, half = self.rows, self.half
        right, left, opp = 1, -1, 2
        if n == 0:
            self.start("d2d")
        elif n == 1:
            self.wait("d2d")
            self.put(0, self.mine(opp, 0, rows))
            if self.direct:
                self.start("io")
                self.put(rows, self.mine(right, 0, rows))
                self.start("ir")
                self.put(2 * rows, self.mine(left, 0, rows))
                self.start("il")
            else:
                self.start("s1a", "s1b")
                self.put(rows + half, self.mine(right, half, rows))
                self.start("ownb")
                self.put(2 * rows, self.mine(left, 0, half))
                self.start("owna")
        elif n == 2:
            self.wait("s1a")
            self.put(rows, self.mine(right, 0, half) + self.got(0, half))
            self.start("reda")
            self.wait("s1b")
            self.put(2 * rows + half, self.mine(left, half, rows) + self.got(half, rows))
            self.start("redb")
        elif n == 3:
            total = self.mine(0, 0, rows)
            if self.direct:
                self.wait("ir", "il", "io")
                total = total + self.got(rows, 2 * rows) + self.got(2 * rows, 3 * rows) + self.got(0, rows)
            else:
                self.wait("ownb", "owna", "reda", "redb")
                total = total + self.got(rows, 2 * rows) + self.got(2 * rows, 3 * rows)
            self.full[pl.ds(self.row(0), rows), :] = self.finish(total)
            if self.gather_direct:
                self.start("go")
            self.start("gr", "gl", "gp")
        elif n == 4:
            self.wait("gr")
            if not self.gather_direct:
                self.start("fa")
            self.start("flp")
            self.wait("gl")
            if not self.gather_direct:
                self.start("fb")
            self.start("frp")
        elif n == 5:
            if self.gather_direct:
                self.wait("go")
            else:
                self.wait("fa", "fb")
            self.start("fop")
        elif n == 6:
            self.wait("gp", "flp", "frp", "fop")

    def drain(self):
        for kind in self.kinds:
            self.copy(kind).wait_send()


def kernel(cfg, theta_hbm, lam_hbm, mu_hbm, ut_hbm, a_hbm, y_hbm, th, tb, av, sa, sb, kb, kv,
           lam_ref, mu_ref, ut_ref, y_ref, load_sem, small_sem, *chunk_bufs):
    chips, band, step, lik = cfg
    n_part, dim = th.shape
    m_rows = av.shape[0]
    nb, mc = n_part // 2, m_rows // 2
    owners = CORES * chips
    own = nb // owners
    wide, sub = dim // 2, 512
    blocks = [[(a, b) for a in (2 * i, 2 * i + 1) for b in range(a + 1)] for i in range(2)]
    share = LANES // owners
    q_row = len(blocks[1]) * share
    g1_piece = q_row + ut_ref.shape[0] // owners * (n_part // LANES)
    rank = ut_ref.shape[0]
    pull = 2.0 / band
    gain = step / n_part
    me = lax.axis_index("feat")
    core, chip = lax.rem(me, CORES), me // CORES
    group = lax.axis_index("ens") * owners
    chip_of = {hop: lax.rem(chip + hop + chips, chips) for hop in (-1, 0, 1, 2)}
    ids = {hop: group + chip_of[hop] * CORES + core for hop in (-1, 1, 2)}
    ids["pair"] = group + chip * CORES + (1 - core)
    where = (core, chip, chips, chip_of, ids)

    def finish(name):
        if name[0] == "g":
            return lambda g: g
        lo = 0 if name in ("z0", "z1") else mc

        def residual(z):
            return (y_ref[:, lo:lo + mc].astype(F32) - 1.0 / (1.0 + jnp.exp(-z))).astype(BF16)
        return residual

    ch = {}
    for k, name in enumerate(CHUNKS):
        ch[name] = Chunk(name, chunk_bufs[7 * k:7 * k + 7], where, finish(name))

    def rows(i):
        return slice(i * nb, (i + 1) * nb)

    def load_theta(i):
        return pltpu.make_async_copy(theta_hbm.at[pl.ds(i * nb, nb), :], th.at[pl.ds(i * nb, nb), :], load_sem.at[i])

    def load_a(j):
        return pltpu.make_async_copy(a_hbm.at[pl.ds(j * mc, mc), :], av.at[pl.ds(j * mc, mc), :], load_sem.at[2 + j])

    load_theta(0).start()
    load_a(0).start()
    load_a(1).start()
    load_theta(1).start()
    small = [pltpu.make_async_copy(src, dst, small_sem.at[k]) for k, (src, dst) in enumerate(
        ((lam_hbm, lam_ref), (mu_hbm, mu_ref), (ut_hbm, ut_ref), (y_hbm, y_ref)))]
    for copy in small:
        copy.start()

    barrier = pltpu.get_barrier_semaphore()
    for peer in ids.values():
        pl.semaphore_signal(barrier, inc=1, device_id=peer, device_id_type=LOGICAL)
    pl.semaphore_wait(barrier, len(ids))

    def columns(lo, hi):
        return [slice(n, n + sub) for n in range(lo, hi, sub)]

    def prep(i):
        load_theta(i).wait()

        @pl.loop(0, dim // wide)
        def _(t):
            n = pl.ds(pl.multiple_of(t * wide, wide), wide)
            tb[rows(i), n] = th[rows(i), n].astype(BF16)

    def project():
        q = jnp.zeros((rank, n_part), F32)
        for n in columns(0, dim):
            q = q + dot(ut_ref[:, n], (th[:, n] - mu_ref[:, n]).astype(BF16), NT)
        part = rank // owners
        for o in range(owners):
            for k in range(n_part // LANES):
                lo = o * g1_piece + q_row + k * part
                ch["g1"].part[lo:lo + part, :] = q[o * part:(o + 1) * part, k * LANES:(k + 1) * LANES]

    def gram(i):
        g = dot(tb[rows(i), :], tb[0:(i + 1) * nb, :], NT)
        part = ch[f"g{i}"].part
        piece = part.shape[0] // owners
        for k, (a, b) in enumerate(blocks[i]):
            block = g[(a - 2 * i) * LANES:(a - 2 * i + 1) * LANES, b * LANES:(b + 1) * LANES]
            for o in range(owners):
                part[o * piece + k * share:o * piece + (k + 1) * share, :] = block[o * share:(o + 1) * share]

    def logit(name, i, j):
        ch[name].part[...] = dot(tb[rows(i), :], av[j * mc:(j + 1) * mc, :], NT)

    def base(i, n, q):
        x = th[rows(i), n] - mu_ref[:, n]
        return x * lam_ref[:, n] + dot(q, ut_ref[:, n]) + pull * tb[rows(i), n].astype(F32)

    def gathered_q(i):
        part = rank // owners
        parts = []
        for k in range(i * nb // LANES, (i + 1) * nb // LANES):
            los = [o * g1_piece + q_row + k * part for o in range(owners)]
            parts.append(jnp.concatenate([ch["g1"].full[lo:lo + part, :] for lo in los], axis=0).T)
        return jnp.concatenate(parts, axis=0).astype(BF16)

    def both_lik(lo, hi):
        for n in columns(lo, hi):
            sa[rows(0), n] = lik * (dot(ch["z0"].full[...], av[0:mc, n]) + dot(ch["z3"].full[...], av[mc:2 * mc, n]))

    def first_lik(lo, hi):
        for n in columns(lo, hi):
            sa[rows(1), n] = lik * dot(ch["z1"].full[...], av[0:mc, n])

    def last_lik(lo, hi):
        for n in columns(lo, hi):
            sb[rows(1), n] = (sa[rows(1), n] + lik * dot(ch["z2"].full[...], av[mc:2 * mc, n])).astype(BF16)

    def low_rank(i):
        q = gathered_q(i)
        for n in columns(0, dim):
            s = sa[rows(i), n] - base(i, n, q)
            if i == 0:
                sb[rows(i), n] = s.astype(BF16)
            else:
                sa[rows(i), n] = s

    def kernel_mat():
        grams = {}
        for i in range(2):
            full = ch[f"g{i}"].full
            piece = full.shape[0] // owners
            for k, ab in enumerate(blocks[i]):
                grams[ab] = jnp.concatenate(
                    [full[o * piece + k * share:o * piece + (k + 1) * share, :] for o in range(owners)], axis=0)
        eye = lax.broadcasted_iota(jnp.int32, (LANES, LANES), 0) == lax.broadcasted_iota(jnp.int32, (LANES, LANES), 1)
        count = n_part // LANES
        norms = [jnp.where(eye, grams[a, a], 0.0) for a in range(count)]
        cols = [jnp.sum(d, axis=1, keepdims=True) for d in norms]
        lines = [jnp.sum(d, axis=0, keepdims=True) for d in norms]
        totals = [0.0] * count
        for (a, b), g in grams.items():
            k = jnp.exp(-jnp.maximum(cols[a] + lines[b] - 2.0 * g, 0.0) / band)
            for i, j, m in ((a, b, k), (b, a, k.T))[:2 if a != b else 1]:
                kb[i * LANES:(i + 1) * LANES, j * LANES:(j + 1) * LANES] = m.astype(BF16)
                totals[i] = totals[i] + jnp.sum(m, axis=1, keepdims=True)
        for a in range(count):
            kv[a * LANES:(a + 1) * LANES, :] = jnp.broadcast_to(gain * pull * totals[a], (LANES, LANES))

    def drive_first(i):
        for n in columns(0, dim):
            t = th[rows(i), n]
            scale = jnp.concatenate([kv[rows(i), :]] * (sub // LANES), axis=1)
            th[rows(i), n] = t + (scale * t + gain * dot(kb[rows(i), rows(0)], sb[rows(0), n]))

    def drive(i, lo, hi):
        for n in columns(lo, hi):
            t = th[rows(i), n] + gain * dot(kb[rows(i), rows(1)], sb[rows(1), n])
            th[rows(i), n] = t
            tb[rows(i), n] = t.astype(BF16)

    halves = {"a": (0, wide), "b": (wide, dim)}
    pieces = {
        "proj": project, "gram0": lambda: gram(0), "gram1": lambda: gram(1),
        "z0p": lambda: logit("z0", 0, 0), "z0q": lambda: logit("z3", 0, 1),
        "z1": lambda: logit("z1", 1, 0), "z2": lambda: logit("z2", 1, 1),
        "lr0": lambda: low_rank(0), "lr1": lambda: low_rank(1), "kmat": kernel_mat,
        "d0": lambda: drive_first(0), "d1": lambda: drive_first(1),
    }
    for h, (lo, hi) in halves.items():
        pieces["l0" + h] = functools.partial(both_lik, lo, hi)
        pieces["lf1" + h] = functools.partial(first_lik, lo, hi)
        pieces["ll1" + h] = functools.partial(last_lik, lo, hi)
        pieces["drive0" + h] = functools.partial(drive, 0, lo, hi)
        pieces["drive1" + h] = functools.partial(drive, 1, lo, hi)

    @pl.loop(0, NUM_STEPS)
    def _(s):
        @pl.when(s == 0)
        def _():
            for copy in small:
                copy.wait()
            prep(0)

        loaded = set()
        for item in SCHEDULE:
            if ":" in item:
                name, n = item.split(":")
                ch[name].stage(int(n))
                continue
            if item in ("z0p", "z0q"):
                @pl.when(s == 0)
                def _():
                    load_a("pq".index(item[-1])).wait()
            if item == "drive1a":
                @pl.when(s == 0)
                def _():
                    prep(1)
            if item[:6] == "drive1":
                pl.when(s > 0)(pieces[item])
            elif item in ("proj", "gram0"):
                pl.when(me >= 0)(pieces[item])
            else:
                pieces[item]()
        for name in CHUNKS:
            ch[name].drain()

    for lo, hi in halves.values():
        drive(1, lo, hi)


def solution(mesh):
    feat_size = mesh.shape["feat"]
    chips = feat_size // CORES

    def local_run(particles, prec_diag, low_factor, prior_mean, data_mat, labels):
        n_part, dim = particles.shape
        m_rows = data_mat.shape[0]
        rank = low_factor.shape[1]
        dim_full = dim * feat_size
        cfg = (chips, 2.0 * dim_full, dim_full / 4.0, 2.0 / math.sqrt(m_rows * dim_full))
        nb, mc = n_part // 2, m_rows // 2
        own = nb // feat_size
        vm, any_ = pl.BlockSpec(memory_space=pltpu.VMEM), pl.BlockSpec(memory_space=pl.ANY)
        dma = pltpu.SemaphoreType.DMA
        scratch = [
            pltpu.VMEM((n_part, dim), BF16), pltpu.VMEM((m_rows, dim), BF16),
            pltpu.VMEM((n_part, dim), F32), pltpu.VMEM((n_part, dim), BF16),
            pltpu.VMEM((n_part, n_part), BF16), pltpu.VMEM((n_part, LANES), F32),
            pltpu.VMEM((1, dim), F32), pltpu.VMEM((1, dim), F32), pltpu.VMEM((rank, dim), BF16),
            pltpu.VMEM((1, m_rows), jnp.int32), dma((4,)), dma((4,)),
        ]
        for name in CHUNKS:
            wire, width, rows = (F32, LANES, own // 2 * 3) if name[0] == "g" else (BF16, mc, own)
            if name == "g1":
                rows = own // 2 * 7 + rank * n_part // LANES // feat_size
            scratch += [
                pltpu.VMEM((feat_size * rows, width), F32), pltpu.VMEM((chips * rows, width), F32),
                pltpu.VMEM((3 * rows, width), wire), pltpu.VMEM((3 * rows, width), wire),
                pltpu.VMEM((feat_size * rows, width), wire), dma((len(KINDS),)), dma((len(KINDS),)),
            ]
        return pl.pallas_call(
            functools.partial(kernel, cfg),
            out_shape=pltpu.VMEM((n_part, dim), F32),
            in_specs=[any_] * 6,
            out_specs=vm,
            scratch_shapes=scratch,
            compiler_params=pltpu.CompilerParams(
                collective_id=0, has_side_effects=True, vmem_limit_bytes=48 * 2**20),
            cost_estimate=pl.CostEstimate(flops=60 * 10**9, bytes_accessed=32 * 2**20, transcendentals=0),
        )(particles, prec_diag[None, :], prior_mean[None, :], low_factor.T, data_mat, labels[None, :])

    return jax.shard_map(
        local_run,
        mesh=mesh,
        in_specs=(P("ens", "feat"), P(("ens", "feat")), P(("ens", "feat"), None),
                  P(("ens", "feat")), P("ens", "feat"), P("ens")),
        out_specs=P("ens", "feat"),
        check_vma=False,
    )
```

```python
import functools
import math
import jax
import jax.numpy as jnp
from jax import lax
from jax.experimental import pallas as pl
from jax.experimental.pallas import tpu as pltpu
from jax.sharding import PartitionSpec as P

NUM_STEPS = 3
CORES = 2
LANES = 128
F32, BF16 = jnp.float32, jnp.bfloat16
NN = (((1,), (0,)), ((), ()))
NT = (((1,), (1,)), ((), ()))
LOGICAL = pl.DeviceIdType.LOGICAL
KINDS = ("d2d", "s1a", "s1b", "ownb", "owna", "reda", "redb", "ir", "il", "io",
         "gr", "gl", "go", "gp", "fa", "flp", "fb", "frp", "fop")
CHUNKS = ("g0", "z0", "z3", "g1", "z1", "z2")
DIRECT = ('z0', 'z3', 'z1', 'z2', 'g0', 'g1')
GATHER_DIRECT = ('z0', 'z3', 'z1', 'z2', 'g0', 'g1')
SCHEDULE = (
    "gram0", "g0:0", "z0p", "z0:0", "drive1a", "g0:1", "z0q", "z3:0", "drive1b", "z0:1", "z1", "z1:0",
    "z3:1", "proj", "z1:1", "gram1", "z0:3", "g1:0", "z3:3", "z2", "z2:0", "g1:1", "z1:3", "z2:1",
    "z3:4", "z3:5", "z0:4", "z0:5", "g1:3", "z1:4", "z3:6", "z0:6", "z1:5", "l0a", "g0:3", "z1:6",
    "z2:3", "lf1a", "lf1b", "l0b", "g1:4", "g1:5", "g0:4", "g0:5", "g1:6", "lr0", "z2:4", "z2:5",
    "lr1", "g0:6", "kmat", "z2:6", "ll1a", "d1", "d0", "ll1b", "drive0a", "drive0b",
)


def dot(a, b, dims=NN):
    return lax.dot_general(a, b, dims, preferred_element_type=F32)


class Chunk:
    def __init__(self, name, bufs, where, finish):
        self.part, self.pair, self.send, self.recv, self.full, self.ssem, self.rsem = bufs
        self.core, self.chip, self.chips, self.chip_of, self.ids = where
        self.rows = self.full.shape[0] // (CORES * self.chips)
        self.half = self.rows // 2 // 16 * 16
        self.direct = name in DIRECT
        self.gather_direct = name in GATHER_DIRECT
        unused = {"s1a", "s1b", "ownb", "owna", "reda", "redb"} if self.direct else {"ir", "il", "io"}
        unused |= {"fa", "fb"} if self.gather_direct else {"go"}
        self.kinds = [kind for kind in KINDS if kind not in unused]
        self.finish = finish

    def row(self, hop):
        return pl.multiple_of((self.core * self.chips + self.chip_of[hop]) * self.rows, 8)

    def copy(self, kind):
        rows, half = self.rows, self.half
        core, pair = self.core, self.ids["pair"]
        chip, right, left, opp = 0, 1, -1, 2
        at = lambda hop: self.ids[hop]
        snd, rcv, full = self.send, self.recv, self.full

        def same(lo, size):
            ref = full.at[pl.ds(lo, size), :]
            return ref, ref

        def slot(lo, hi):
            return snd.at[pl.ds(lo, hi - lo), :], rcv.at[pl.ds(lo, hi - lo), :]

        if kind == "d2d":
            size = self.chips * rows
            src, dst = self.part.at[pl.ds(pl.multiple_of((1 - core) * size, 8), size), :], self.pair
            dev = pair
        else:
            (src, dst), dev = {
                "s1a": lambda: (slot(0, half), at(right)),
                "s1b": lambda: (slot(half, rows), at(left)),
                "ownb": lambda: (slot(rows + half, 2 * rows), at(right)),
                "owna": lambda: (slot(2 * rows, 2 * rows + half), at(left)),
                "reda": lambda: (slot(rows, rows + half), at(right)),
                "redb": lambda: (slot(2 * rows + half, 3 * rows), at(left)),
                "io": lambda: (slot(0, rows), at(opp)),
                "ir": lambda: (slot(rows, 2 * rows), at(right)),
                "il": lambda: (slot(2 * rows, 3 * rows), at(left)),
                "gr": lambda: (same(self.row(chip), rows), at(right)),
                "gl": lambda: (same(self.row(chip), rows), at(left)),
                "go": lambda: (same(self.row(chip), rows), at(opp)),
                "gp": lambda: (same(self.row(chip), rows), pair),
                "fa": lambda: (same(self.row(left), half), at(right)),
                "flp": lambda: (same(self.row(left), rows), pair),
                "fb": lambda: (same(self.row(right) + half, rows - half), at(left)),
                "frp": lambda: (same(self.row(right), rows), pair),
                "fop": lambda: (same(self.row(opp), rows), pair),
            }[kind]()
        k = KINDS.index(kind)
        return pltpu.make_async_remote_copy(
            src_ref=src, dst_ref=dst, send_sem=self.ssem.at[k], recv_sem=self.rsem.at[k],
            device_id=dev, device_id_type=LOGICAL)

    def start(self, *kinds):
        for kind in kinds:
            self.copy(kind).start()

    def wait(self, *kinds):
        for kind in kinds:
            self.copy(kind).wait_recv()

    def mine(self, hop, lo, hi):
        a = self.part[pl.ds(self.row(hop) + lo, hi - lo), :]
        b = self.pair[pl.ds(pl.multiple_of(self.chip_of[hop] * self.rows, 8) + lo, hi - lo), :]
        return a + b

    def put(self, lo, value):
        self.send[lo:lo + value.shape[0], :] = value.astype(self.send.dtype)

    def got(self, lo, hi):
        return self.recv[lo:hi, :].astype(F32)

    def stage(self, n):
        rows, half = self.rows, self.half
        right, left, opp = 1, -1, 2
        if n == 0:
            self.start("d2d")
        elif n == 1:
            self.wait("d2d")
            self.put(0, self.mine(opp, 0, rows))
            if self.direct:
                self.start("io")
                self.put(rows, self.mine(right, 0, rows))
                self.start("ir")
                self.put(2 * rows, self.mine(left, 0, rows))
                self.start("il")
            else:
                self.start("s1a", "s1b")
                self.put(rows + half, self.mine(right, half, rows))
                self.start("ownb")
                self.put(2 * rows, self.mine(left, 0, half))
                self.start("owna")
        elif n == 2:
            self.wait("s1a")
            self.put(rows, self.mine(right, 0, half) + self.got(0, half))
            self.start("reda")
            self.wait("s1b")
            self.put(2 * rows + half, self.mine(left, half, rows) + self.got(half, rows))
            self.start("redb")
        elif n == 3:
            total = self.mine(0, 0, rows)
            if self.direct:
                self.wait("ir", "il", "io")
                total = total + self.got(rows, 2 * rows) + self.got(2 * rows, 3 * rows) + self.got(0, rows)
            else:
                self.wait("ownb", "owna", "reda", "redb")
                total = total + self.got(rows, 2 * rows) + self.got(2 * rows, 3 * rows)
            self.full[pl.ds(self.row(0), rows), :] = self.finish(total)
            if self.gather_direct:
                self.start("go")
            self.start("gr", "gl", "gp")
        elif n == 4:
            self.wait("gr")
            if not self.gather_direct:
                self.start("fa")
            self.start("flp")
            self.wait("gl")
            if not self.gather_direct:
                self.start("fb")
            self.start("frp")
        elif n == 5:
            if self.gather_direct:
                self.wait("go")
            else:
                self.wait("fa", "fb")
            self.start("fop")
        elif n == 6:
            self.wait("gp", "flp", "frp", "fop")

    def drain(self):
        for kind in self.kinds:
            self.copy(kind).wait_send()


def kernel(cfg, theta_hbm, lam_hbm, mu_hbm, ut_hbm, a_hbm, y_hbm, th, tb, av, sa, sb, kb, kv,
           lam_ref, mu_ref, ut_ref, y_ref, load_sem, small_sem, *chunk_bufs):
    chips, band, step, lik = cfg
    n_part, dim = th.shape
    m_rows = av.shape[0]
    nb, mc = n_part // 2, m_rows // 2
    owners = CORES * chips
    own = nb // owners
    wide, sub = dim // 2, 512
    blocks = [[(a, b) for a in (2 * i, 2 * i + 1) for b in range(a + 1)] for i in range(2)]
    share = LANES // owners
    q_row = len(blocks[1]) * share
    g1_piece = q_row + ut_ref.shape[0] // owners * (n_part // LANES)
    rank = ut_ref.shape[0]
    pull = 2.0 / band
    gain = step / n_part
    me = lax.axis_index("feat")
    core, chip = lax.rem(me, CORES), me // CORES
    group = lax.axis_index("ens") * owners
    chip_of = {hop: lax.rem(chip + hop + chips, chips) for hop in (-1, 0, 1, 2)}
    ids = {hop: group + chip_of[hop] * CORES + core for hop in (-1, 1, 2)}
    ids["pair"] = group + chip * CORES + (1 - core)
    where = (core, chip, chips, chip_of, ids)

    def finish(name):
        if name[0] == "g":
            return lambda g: g
        lo = 0 if name in ("z0", "z1") else mc

        def residual(z):
            return (y_ref[:, lo:lo + mc].astype(F32) - 1.0 / (1.0 + jnp.exp(-z))).astype(BF16)
        return residual

    ch = {}
    for k, name in enumerate(CHUNKS):
        ch[name] = Chunk(name, chunk_bufs[7 * k:7 * k + 7], where, finish(name))

    def rows(i):
        return slice(i * nb, (i + 1) * nb)

    def load_theta(i):
        return pltpu.make_async_copy(theta_hbm.at[pl.ds(i * nb, nb), :], th.at[pl.ds(i * nb, nb), :], load_sem.at[i])

    def load_a(j):
        return pltpu.make_async_copy(a_hbm.at[pl.ds(j * mc, mc), :], av.at[pl.ds(j * mc, mc), :], load_sem.at[2 + j])

    load_theta(0).start()
    load_a(0).start()
    load_a(1).start()
    load_theta(1).start()
    small = [pltpu.make_async_copy(src, dst, small_sem.at[k]) for k, (src, dst) in enumerate(
        ((lam_hbm, lam_ref), (mu_hbm, mu_ref), (ut_hbm, ut_ref), (y_hbm, y_ref)))]
    for copy in small:
        copy.start()

    barrier = pltpu.get_barrier_semaphore()
    for peer in ids.values():
        pl.semaphore_signal(barrier, inc=1, device_id=peer, device_id_type=LOGICAL)
    pl.semaphore_wait(barrier, len(ids))

    def columns(lo, hi):
        return [slice(n, n + sub) for n in range(lo, hi, sub)]

    def prep(i):
        load_theta(i).wait()

        @pl.loop(0, dim // wide)
        def _(t):
            n = pl.ds(pl.multiple_of(t * wide, wide), wide)
            tb[rows(i), n] = th[rows(i), n].astype(BF16)

    def project():
        q = jnp.zeros((rank, n_part), F32)
        for n in columns(0, dim):
            q = q + dot(ut_ref[:, n], (th[:, n] - mu_ref[:, n]).astype(BF16), NT)
        part = rank // owners
        for o in range(owners):
            for k in range(n_part // LANES):
                lo = o * g1_piece + q_row + k * part
                ch["g1"].part[lo:lo + part, :] = q[o * part:(o + 1) * part, k * LANES:(k + 1) * LANES]

    def gram(i):
        g = dot(tb[rows(i), :], tb[0:(i + 1) * nb, :], NT)
        part = ch[f"g{i}"].part
        piece = part.shape[0] // owners
        for k, (a, b) in enumerate(blocks[i]):
            block = g[(a - 2 * i) * LANES:(a - 2 * i + 1) * LANES, b * LANES:(b + 1) * LANES]
            for o in range(owners):
                part[o * piece + k * share:o * piece + (k + 1) * share, :] = block[o * share:(o + 1) * share]

    def logit(name, i, j):
        ch[name].part[...] = dot(tb[rows(i), :], av[j * mc:(j + 1) * mc, :], NT)

    def base(i, n, q):
        x = th[rows(i), n] - mu_ref[:, n]
        return x * lam_ref[:, n] + dot(q, ut_ref[:, n]) + pull * tb[rows(i), n].astype(F32)

    def gathered_q(i):
        part = rank // owners
        parts = []
        for k in range(i * nb // LANES, (i + 1) * nb // LANES):
            los = [o * g1_piece + q_row + k * part for o in range(owners)]
            parts.append(jnp.concatenate([ch["g1"].full[lo:lo + part, :] for lo in los], axis=0).T)
        return jnp.concatenate(parts, axis=0).astype(BF16)

    def both_lik(lo, hi):
        for n in columns(lo, hi):
            sa[rows(0), n] = lik * (dot(ch["z0"].full[...], av[0:mc, n]) + dot(ch["z3"].full[...], av[mc:2 * mc, n]))

    def first_lik(lo, hi):
        for n in columns(lo, hi):
            sa[rows(1), n] = lik * dot(ch["z1"].full[...], av[0:mc, n])

    def last_lik(lo, hi):
        for n in columns(lo, hi):
            sb[rows(1), n] = (sa[rows(1), n] + lik * dot(ch["z2"].full[...], av[mc:2 * mc, n])).astype(BF16)

    def low_rank(i):
        q = gathered_q(i)
        for n in columns(0, dim):
            s = sa[rows(i), n] - base(i, n, q)
            if i == 0:
                sb[rows(i), n] = s.astype(BF16)
            else:
                sa[rows(i), n] = s

    def kernel_mat():
        grams = {}
        for i in range(2):
            full = ch[f"g{i}"].full
            piece = full.shape[0] // owners
            for k, ab in enumerate(blocks[i]):
                grams[ab] = jnp.concatenate(
                    [full[o * piece + k * share:o * piece + (k + 1) * share, :] for o in range(owners)], axis=0)
        eye = lax.broadcasted_iota(jnp.int32, (LANES, LANES), 0) == lax.broadcasted_iota(jnp.int32, (LANES, LANES), 1)
        count = n_part // LANES
        norms = [jnp.where(eye, grams[a, a], 0.0) for a in range(count)]
        cols = [jnp.sum(d, axis=1, keepdims=True) for d in norms]
        lines = [jnp.sum(d, axis=0, keepdims=True) for d in norms]
        totals = [0.0] * count
        for (a, b), g in grams.items():
            k = jnp.exp(-jnp.maximum(cols[a] + lines[b] - 2.0 * g, 0.0) / band)
            for i, j, m in ((a, b, k), (b, a, k.T))[:2 if a != b else 1]:
                kb[i * LANES:(i + 1) * LANES, j * LANES:(j + 1) * LANES] = m.astype(BF16)
                totals[i] = totals[i] + jnp.sum(m, axis=1, keepdims=True)
        for a in range(count):
            kv[a * LANES:(a + 1) * LANES, :] = jnp.broadcast_to(gain * pull * totals[a], (LANES, LANES))

    def drive_first(i):
        for n in columns(0, dim):
            t = th[rows(i), n]
            scale = jnp.concatenate([kv[rows(i), :]] * (sub // LANES), axis=1)
            th[rows(i), n] = t + (scale * t + gain * dot(kb[rows(i), rows(0)], sb[rows(0), n]))

    def drive(i, lo, hi):
        for n in columns(lo, hi):
            t = th[rows(i), n] + gain * dot(kb[rows(i), rows(1)], sb[rows(1), n])
            th[rows(i), n] = t
            tb[rows(i), n] = t.astype(BF16)

    halves = {"a": (0, wide), "b": (wide, dim)}
    pieces = {
        "proj": project, "gram0": lambda: gram(0), "gram1": lambda: gram(1),
        "z0p": lambda: logit("z0", 0, 0), "z0q": lambda: logit("z3", 0, 1),
        "z1": lambda: logit("z1", 1, 0), "z2": lambda: logit("z2", 1, 1),
        "lr0": lambda: low_rank(0), "lr1": lambda: low_rank(1), "kmat": kernel_mat,
        "d0": lambda: drive_first(0), "d1": lambda: drive_first(1),
    }
    for h, (lo, hi) in halves.items():
        pieces["l0" + h] = functools.partial(both_lik, lo, hi)
        pieces["lf1" + h] = functools.partial(first_lik, lo, hi)
        pieces["ll1" + h] = functools.partial(last_lik, lo, hi)
        pieces["drive0" + h] = functools.partial(drive, 0, lo, hi)
        pieces["drive1" + h] = functools.partial(drive, 1, lo, hi)

    @pl.loop(0, NUM_STEPS)
    def _(s):
        @pl.when(s == 0)
        def _():
            for copy in small:
                copy.wait()
            prep(0)

        loaded = set()
        for item in SCHEDULE:
            if ":" in item:
                name, n = item.split(":")
                ch[name].stage(int(n))
                continue
            if item in ("z0p", "z0q"):
                @pl.when(s == 0)
                def _():
                    load_a("pq".index(item[-1])).wait()
            if item == "drive1a":
                @pl.when(s == 0)
                def _():
                    prep(1)
            if item[:6] == "drive1":
                pl.when(s > 0)(pieces[item])
            else:
                pieces[item]()
        for name in CHUNKS:
            ch[name].drain()

    for lo, hi in halves.values():
        drive(1, lo, hi)


def solution(mesh):
    feat_size = mesh.shape["feat"]
    chips = feat_size // CORES

    def local_run(particles, prec_diag, low_factor, prior_mean, data_mat, labels):
        n_part, dim = particles.shape
        m_rows = data_mat.shape[0]
        rank = low_factor.shape[1]
        dim_full = dim * feat_size
        cfg = (chips, 2.0 * dim_full, dim_full / 4.0, 2.0 / math.sqrt(m_rows * dim_full))
        nb, mc = n_part // 2, m_rows // 2
        own = nb // feat_size
        vm, any_ = pl.BlockSpec(memory_space=pltpu.VMEM), pl.BlockSpec(memory_space=pl.ANY)
        dma = pltpu.SemaphoreType.DMA
        scratch = [
            pltpu.VMEM((n_part, dim), BF16), pltpu.VMEM((m_rows, dim), BF16),
            pltpu.VMEM((n_part, dim), F32), pltpu.VMEM((n_part, dim), BF16),
            pltpu.VMEM((n_part, n_part), BF16), pltpu.VMEM((n_part, LANES), F32),
            pltpu.VMEM((1, dim), F32), pltpu.VMEM((1, dim), F32), pltpu.VMEM((rank, dim), BF16),
            pltpu.VMEM((1, m_rows), jnp.int32), dma((4,)), dma((4,)),
        ]
        for name in CHUNKS:
            wire, width, rows = (F32, LANES, own // 2 * 3) if name[0] == "g" else (BF16, mc, own)
            if name == "g1":
                rows = own // 2 * 7 + rank * n_part // LANES // feat_size
            scratch += [
                pltpu.VMEM((feat_size * rows, width), F32), pltpu.VMEM((chips * rows, width), F32),
                pltpu.VMEM((3 * rows, width), wire), pltpu.VMEM((3 * rows, width), wire),
                pltpu.VMEM((feat_size * rows, width), wire), dma((len(KINDS),)), dma((len(KINDS),)),
            ]
        return pl.pallas_call(
            functools.partial(kernel, cfg),
            out_shape=pltpu.VMEM((n_part, dim), F32),
            in_specs=[any_] * 6,
            out_specs=vm,
            scratch_shapes=scratch,
            compiler_params=pltpu.CompilerParams(
                collective_id=0, has_side_effects=True, vmem_limit_bytes=48 * 2**20),
            cost_estimate=pl.CostEstimate(flops=60 * 10**9, bytes_accessed=32 * 2**20, transcendentals=0),
        )(particles, prec_diag[None, :], prior_mean[None, :], low_factor.T, data_mat, labels[None, :])

    return jax.shard_map(
        local_run,
        mesh=mesh,
        in_specs=(P("ens", "feat"), P(("ens", "feat")), P(("ens", "feat"), None),
                  P(("ens", "feat")), P("ens", "feat"), P("ens")),
        out_specs=P("ens", "feat"),
        check_vma=False,
    )
```
